128 devices in a mesh: cp: 64 (over x, z, y), hd: 2 (over core).
Axes of the slice: x: 4, y: 4, z: 4, core: 2. Of those that a mesh axis runs over, the one named last changes fastest.
Arguments:
- queries: bfloat16 [12288, 4096], P('cp', 'hd'), may hold values from -48 to 48
- keys: bfloat16 [12288, 1024], P('cp', 'hd'), may hold values from -48 to 48
- values: bfloat16 [12288, 1024], P('cp', 'hd'), may hold values from -6 to 6
- span_table: int32 [128], replicated, may hold values from 0 to 127, as said below
- doc_ids: int32 [12288], replicated, may hold values from 0 to 7, never falling along the last dimension, each value on 1 to 3072 neighbouring positions
- out_weight: bfloat16 [4096, 4096], P('hd'), may hold values from -0.09375 to 0.09375
Outputs:
- mixed: bfloat16 [12288, 4096], P(('cp', 'hd'))
The draws below stay inside these ranges and needn't reach their ends.
Inputs may be any that keep to these rules, and one draw needn't show every extreme that they name: `span_table`: slots 2 j and 2 j + 1 hold two spans c and 127 - c, and every span is held once.
All inputs are finite; a program needn't handle non-finite values.
Results may differ from the reference program's by a relative error of at most 0.0095.
Values may be sent and summed in bfloat16 or wider, within the bound.
No kernel may reach another device: no remote copies, remote signals or barrier semaphores. Data moves between devices by JAX's collectives and lax.ppermute only.
A program may use at most 128 MiB of HBM per device.

```python
import math
import jax
import jax.numpy as jnp
import numpy as np
from jax import lax

D = 4096
QUERY_HEADS = 32
KEY_VALUE_HEADS = 8
HEAD_WIDTH = 128
SPAN_TOKENS = 96
DOCS = 8
SPANS = 128
SEQUENCE_TOKENS = 12288


def paired_table(key):
    pairs = jax.random.permutation(jax.random.fold_in(key, 11), SPANS // 2).astype(jnp.int32)
    flips = jax.random.randint(jax.random.fold_in(key, 12), (SPANS // 2,), 0, 2)
    upper = (SPANS - 1 - pairs).astype(jnp.int32)
    first = jnp.where(flips == 1, upper, pairs)
    second = jnp.where(flips == 1, pairs, upper)
    return jnp.stack([first, second], axis=1).reshape(SPANS).astype(jnp.int32)


def draw_span_table(key, part):
    return paired_table(key)


def drawn_pair(key):
    drawn_key_rows = jnp.clip(jax.random.normal(jax.random.fold_in(key, 21), (SEQUENCE_TOKENS, KEY_VALUE_HEADS * HEAD_WIDTH), jnp.float32), -6.0, 6.0)
    base_queries = jnp.clip(jax.random.normal(jax.random.fold_in(key, 22), (SEQUENCE_TOKENS, QUERY_HEADS * HEAD_WIDTH), jnp.float32), -6.0, 6.0)
    new_keys = drawn_key_rows
    new_queries = base_queries
    return (jnp.clip(new_queries, -48.0, 48.0), jnp.clip(new_keys, -48.0, 48.0))


def draw_queries(key, part):
    return drawn_pair(key)[0].astype(jnp.bfloat16)


def draw_keys(key, part):
    return drawn_pair(key)[1].astype(jnp.bfloat16)


def block_levels(rng, dims, shards, smallest, high):
    def one(dim, blocks):
        steps = jax.random.uniform(jax.random.fold_in(jax.random.fold_in(rng, 6), dim), (blocks,), jnp.float32, smallest / len(shards), high / len(shards))
        return jnp.repeat(jnp.exp(steps), dims[dim] // blocks).reshape((-1,) + (1,) * (len(dims) - dim - 1))

    gain = one(*shards[0])
    for cut in shards[1:]:
        gain = gain * one(*cut)
    return gain


def split_up(amount, total, bound, slope):
    portions = [(1 << 20) // math.isqrt(rank ** slope) + 1 for rank in range(2, amount + 1)]
    surplus, given = total - bound - (amount - 1), [1] * (amount - 1)
    while surplus > 0:
        movable = [i for i in range(amount - 1) if given[i] < bound]
        pool, left = sum([portions[i] for i in movable]), surplus
        for i in movable:
            extra = min(bound - given[i], max(1, left * portions[i] // pool), surplus)
            given[i] = given[i] + extra
            surplus = surplus - extra
    return np.array([bound] + given)


def ragged_sizes(own_key, count, total, limit, lean):
    if count == 2:
        one = jax.random.randint(own_key, (), max(1, total - limit), min(limit, total - 1) + 1)
        return jnp.stack([one, total - one])
    sizes = jnp.asarray(split_up(count, total, limit, lean), jnp.int32)
    twos = (count - 1) // 2
    source_of, taker = sizes[1:1 + 2 * twos:2], sizes[2:2 + 2 * twos:2]
    room = jnp.minimum(source_of - 1, limit - taker)
    moved = jax.random.randint(jax.random.fold_in(own_key, 1), (twos,), 0, 1 << 20) % (room + 1)
    sizes = sizes.at[1:1 + 2 * twos:2].set(source_of - moved).at[2:2 + 2 * twos:2].set(taker + moved)
    return sizes[jax.random.permutation(jax.random.fold_in(own_key, 2), count)]


def centred(key, dims, width, bound, cuts=(), kind=jnp.bfloat16):
    gain = block_levels(key, dims, cuts, -0.22, 0.18) if cuts else 1.0
    values = jax.random.normal(key, dims, jnp.float32) * width * gain
    return jnp.minimum(jnp.maximum(values, -bound), bound).astype(kind)


def setup_inputs(seed: int = 0) -> dict:
    seeds = jax.random.split(jax.random.key(seed), 7)
    return {
        "queries": draw_queries(jax.random.fold_in(seeds[6], 71), 0),
        "keys": draw_keys(jax.random.fold_in(seeds[6], 71), 0),
        "values": centred(seeds[2], (SEQUENCE_TOKENS, KEY_VALUE_HEADS * HEAD_WIDTH), 1.0, 6.0, ((0, 64), (1, 2))),
        "span_table": draw_span_table(jax.random.fold_in(seeds[6], 71), 0),
        "doc_ids": jnp.searchsorted(jnp.cumsum(ragged_sizes(seeds[4], DOCS, SEQUENCE_TOKENS, SEQUENCE_TOKENS // 4, 2)), jnp.arange(SEQUENCE_TOKENS), side="right").astype(jnp.int32),
        "out_weight": centred(seeds[5], (QUERY_HEADS * HEAD_WIDTH, D), (QUERY_HEADS * HEAD_WIDTH) ** -0.5, 0.09375, ((0, 2),)),
    }


def reference(queries, keys, values, span_table, doc_ids, out_weight):
    query_group = QUERY_HEADS // KEY_VALUE_HEADS
    scale = HEAD_WIDTH ** -0.5
    rows = jnp.arange(SEQUENCE_TOKENS, dtype=jnp.int32)
    positions = (span_table[rows // SPAN_TOKENS] * SPAN_TOKENS + rows % SPAN_TOKENS).astype(jnp.int32)
    documents = doc_ids[positions]
    key_head_rows = keys.reshape(SEQUENCE_TOKENS, KEY_VALUE_HEADS, HEAD_WIDTH).astype(jnp.float32)
    value_head_rows = values.reshape(SEQUENCE_TOKENS, KEY_VALUE_HEADS, HEAD_WIDTH).astype(jnp.float32)

    def block(index):
        first = (index * SPAN_TOKENS).astype(jnp.int32)
        query_matrix = lax.dynamic_slice_in_dim(queries, first, SPAN_TOKENS, 0)
        query_matrix = query_matrix.reshape(SPAN_TOKENS, KEY_VALUE_HEADS, query_group, HEAD_WIDTH).astype(jnp.float32)
        query_pos = lax.dynamic_slice_in_dim(positions, first, SPAN_TOKENS, 0)
        query_doc = lax.dynamic_slice_in_dim(documents, first, SPAN_TOKENS, 0)
        visible = (positions[None, :] <= query_pos[:, None]) & (documents[None, :] == query_doc[:, None])
        scores = jnp.einsum("qkgd,nkd->kgqn", query_matrix, key_head_rows) * scale
        scores = jnp.where(visible, scores, -1e30)
        best = jnp.max(scores, axis=-1, keepdims=True)
        weights = jnp.where(visible, jnp.exp(scores - best), 0.0)
        denom = jnp.sum(weights, axis=-1)
        rounded = lax.optimization_barrier(weights.astype(jnp.bfloat16)).astype(jnp.float32)
        numer = jnp.einsum("kgqn,nkd->kgqd", rounded, value_head_rows)
        result = numer / denom[..., None]
        return result.transpose(2, 0, 1, 3).reshape(SPAN_TOKENS, QUERY_HEADS * HEAD_WIDTH).astype(jnp.bfloat16)

    attn = lax.map(block, jnp.arange(SEQUENCE_TOKENS // SPAN_TOKENS, dtype=jnp.int32)).reshape(SEQUENCE_TOKENS, QUERY_HEADS * HEAD_WIDTH)
    return jnp.dot(attn, out_weight, preferred_element_type=jnp.float32).astype(jnp.bfloat16)
```

```python
import jax
import jax.numpy as jnp
from jax import lax
from jax.experimental import pallas as pl
from jax.experimental.pallas import tpu as pltpu
from jax.sharding import Mesh, PartitionSpec as P

HEAD = 128
SPAN = 96
CHUNK = 512
RING = 4
LOG2E = 1.4426950408889634


def shift(value, axis, by):
    return lax.ppermute(value, axis, [(i, (i + by) % RING) for i in range(RING)])


def attention_kernel(coords, table, starts, q0, q1, q2, q3, *rest):
    pieces = rest[:16]
    outs = rest[16:20]
    kv, q_all, o_all, sem = rest[20:]
    x, z, y = coords[0], coords[1], coords[2]
    span_total = table.shape[0]
    seq = span_total * SPAN
    group = 4

    def slot_of(dx, dz, dy, half):
        return 2 * (((x + RING - dx) % RING) * 16 + ((z + RING - dz) % RING) * 4 + (y + RING - dy) % RING) + half

    order = [(0, 0), (0, 1), (1, 0), (1, 1), (3, 0), (3, 1), (2, 0), (2, 1)]
    for family in range(2):
        for index, (far, high) in enumerate(order):
            ref = pieces[family * 8 + index]
            for i in range(8):
                near = 2 * high + i // 4
                dy = 2 * family + (i // 2) % 2
                dx, dz = (far, near) if family == 0 else (near, far)
                row = table[slot_of(dx, dz, dy, i % 2)] * SPAN
                pltpu.make_async_copy(
                    ref.at[pl.ds(i * SPAN, SPAN)],
                    kv.at[pl.ds(pl.multiple_of(row, SPAN), SPAN)],
                    sem,
                ).start()

    for s, ref in enumerate((q0, q1, q2, q3)):
        for half in range(2):
            for h in range(group):
                q_all[2 * s + half, h * SPAN : (h + 1) * SPAN, :] = ref[
                    half * SPAN : (half + 1) * SPAN, h * HEAD : (h + 1) * HEAD
                ]

    pltpu.make_async_copy(kv, kv, sem).wait()

    rows = group * SPAN
    factor = HEAD ** -0.5 * LOG2E
    ones = jnp.ones((CHUNK, HEAD), jnp.bfloat16)

    def doc_start(pos):
        best = starts[0]
        for d in range(1, 8):
            best = jnp.where(starts[d] <= pos, starts[d], best)
        return best

    def one_span(i, _):
        span = table[2 * (x * 16 + z * 4 + (y + RING - i // 2) % RING) + i % 2]
        first = span * SPAN
        end = first + SPAN
        q = q_all[i]
        row = lax.broadcasted_iota(jnp.int32, (rows, 1), 0) % SPAN
        pos = first + row
        low = jnp.full((rows, 1), starts[0], jnp.int32)
        for d in range(1, 8):
            low = jnp.where(starts[d] <= pos, starts[d], low)
        low_min = doc_start(first)
        low_max = doc_start(end - 1)
        count = (end - low_min + CHUNK - 1) // CHUNK
        full = jnp.maximum((end - low_max) // CHUNK, 1)

        def scores(k0):
            k = kv[pl.ds(k0, CHUNK), :HEAD]
            return lax.dot_general(q, k, (((1,), (1,)), ((), ())), preferred_element_type=jnp.float32)

        def absorb(s, k0, state):
            best, acc = state
            new_best = jnp.maximum(best, jnp.max(s, axis=1, keepdims=True))
            fade = jnp.exp2((best - new_best) * factor)
            w = jnp.exp2((s - new_best) * factor).astype(jnp.bfloat16)
            v = jnp.concatenate([kv[pl.ds(k0, CHUNK), HEAD:], ones], axis=1)
            return new_best, acc * fade + jnp.dot(w, v, preferred_element_type=jnp.float32)

        def plain(e, state):
            k0 = pl.multiple_of(end - (e + 1) * CHUNK, 32)
            return absorb(scores(k0), k0, state)

        def masked(j, state):
            e = jnp.where(j == 0, 0, full + j - 1)
            upper = end - e * CHUNK
            k0 = pl.multiple_of(jnp.maximum(upper - CHUNK, 0), 32)
            kpos = k0 + lax.broadcasted_iota(jnp.int32, (rows, CHUNK), 1)
            s = scores(k0)
            high = jnp.minimum(pos, upper - 1)
            s = jnp.where((kpos >= low) & (kpos <= high), s, -1e30)
            return absorb(s, k0, state)

        state = (jnp.full((rows, 1), -1e30, jnp.float32), jnp.zeros((rows, 2 * HEAD), jnp.float32))
        state = lax.fori_loop(1, full, plain, state)
        state = lax.fori_loop(0, jnp.maximum(count - full, 0) + 1, masked, state)
        acc = state[1]
        o_all[i] = (acc[:, :HEAD] / acc[:, HEAD:]).astype(jnp.bfloat16)
        return 0

    lax.fori_loop(0, 8, one_span, 0)
    for s, ref in enumerate(outs):
        for half in range(2):
            for h in range(group):
                ref[half * SPAN : (half + 1) * SPAN, h * HEAD : (h + 1) * HEAD] = o_all[
                    2 * s + half, h * SPAN : (h + 1) * SPAN, :
                ]


def attention(coords, table, starts, q_parts, pieces):
    smem = pl.BlockSpec(memory_space=pltpu.SMEM)
    vmem = pl.BlockSpec(memory_space=pltpu.VMEM)
    hbm = pl.BlockSpec(memory_space=pl.ANY)
    seq = table.shape[0] * SPAN
    return pl.pallas_call(
        attention_kernel,
        out_shape=[jax.ShapeDtypeStruct((2 * SPAN, 4 * HEAD), jnp.bfloat16)] * 4,
        in_specs=[smem] * 3 + [vmem] * 4 + [hbm] * 16,
        out_specs=[vmem] * 4,
        scratch_shapes=[
            pltpu.VMEM((seq, 2 * HEAD), jnp.bfloat16),
            pltpu.VMEM((8, 4 * SPAN, HEAD), jnp.bfloat16),
            pltpu.VMEM((8, 4 * SPAN, HEAD), jnp.bfloat16),
            pltpu.SemaphoreType.DMA,
        ],
        compiler_params=pltpu.CompilerParams(vmem_limit_bytes=32 * 1024 * 1024),
        cost_estimate=pl.CostEstimate(flops=6_000_000_000, bytes_accessed=8_000_000, transcendentals=10_000_000),
        name="attention",
    )(coords, table, starts, *q_parts, *pieces)


def project_kernel(coords, o0, o1, o2, o3, w, keep, send, scr):
    y, core = coords[2], coords[3]
    acc = None
    for s, ref in enumerate((o0, o1, o2, o3)):
        first = pl.multiple_of(((y + s) % RING) * 512, 512)
        part = jnp.dot(ref[...], w[pl.ds(first, 512), :], preferred_element_type=jnp.float32)
        acc = part if acc is None else acc + part
    scr[...] = acc
    keep[...] = scr[pl.ds(pl.multiple_of(core * SPAN, SPAN), SPAN), :]
    send[...] = scr[pl.ds(pl.multiple_of((1 - core) * SPAN, SPAN), SPAN), :].astype(jnp.bfloat16)


def project(coords, o_parts, weight, first, width):
    block = 512
    smem = pl.BlockSpec(memory_space=pltpu.SMEM)
    whole = pl.BlockSpec((2 * SPAN, 512), lambda n: (0, 0))
    out = pl.BlockSpec((SPAN, block), lambda n: (0, n))
    return pl.pallas_call(
        project_kernel,
        grid=(width // block,),
        out_shape=[
            jax.ShapeDtypeStruct((SPAN, width), jnp.float32),
            jax.ShapeDtypeStruct((SPAN, width), jnp.bfloat16),
        ],
        in_specs=[smem] + [whole] * 4 + [pl.BlockSpec((weight.shape[0], block), lambda n: (0, n + first // block))],
        out_specs=[out, out],
        scratch_shapes=[pltpu.VMEM((2 * SPAN, block), jnp.float32)],
        compiler_params=pltpu.CompilerParams(vmem_limit_bytes=24 * 1024 * 1024),
        cost_estimate=pl.CostEstimate(
            flops=2 * 192 * 2048 * width, bytes_accessed=2048 * width * 2, transcendentals=0
        ),
        name="project",
    )(coords, *o_parts, weight)


def local(queries, keys, values, span_table, doc_ids, out_weight):
    rows = queries.shape[0]
    x, z, y, core = (lax.axis_index(a) for a in ("x", "z", "y", "hd"))
    coords = jnp.stack([x, z, y, core]).astype(jnp.int32)
    kv = jnp.concatenate([keys.reshape(rows, RING, HEAD), values.reshape(rows, RING, HEAD)], axis=2)
    kv = kv.transpose(1, 0, 2)
    part = [lax.dynamic_index_in_dim(kv, (y + s) % RING, 0, keepdims=False) for s in range(RING)]
    part = [part[0]] + [shift(part[s], "y", s) for s in range(1, RING)]
    low, high = jnp.concatenate(part[:2], 0), jnp.concatenate(part[2:], 0)

    def gathered(block, near_axis, far_axis):
        near = [block] + [shift(block, near_axis, s) for s in range(1, RING)]
        first, second = jnp.concatenate(near[:2], 0), jnp.concatenate(near[2:], 0)
        ahead_first = shift(first, far_axis, 1)
        behind_second = shift(second, far_axis, -1)
        ahead_second = shift(second, far_axis, 1)
        behind_first = shift(first, far_axis, -1)
        far_first = shift(ahead_first, far_axis, 1)
        far_second = shift(behind_second, far_axis, -1)
        return [first, second, ahead_first, ahead_second, behind_first, behind_second, far_first, far_second]

    pieces = gathered(low, "z", "x") + gathered(high, "x", "z")

    q_part = [
        lax.dynamic_slice_in_dim(queries, ((y + s) % RING) * 512, 512, 1) for s in range(RING)
    ]
    q_part = [q_part[0]] + [shift(q_part[s], "y", s) for s in range(1, RING)]
    docs = jnp.arange(8, dtype=jnp.int32)
    starts = jnp.sum((doc_ids[None, :] < docs[:, None]).astype(jnp.int32), axis=1)

    o_part = attention(coords, span_table, starts, q_part, pieces)
    o_part = [o_part[0]] + [shift(o_part[s], "y", -s) for s in range(1, RING)]

    mixed = []
    width = out_weight.shape[1] // 2
    for n in range(2):
        keep, send = project(coords, o_part, out_weight, n * width, width)
        arrived = lax.ppermute(send, "hd", [(0, 1), (1, 0)])
        mixed.append((keep + arrived.astype(jnp.float32)).astype(jnp.bfloat16))
    return jnp.concatenate(mixed, axis=1)


def solution(mesh):
    inner = Mesh(mesh.devices.reshape(RING, RING, RING, 2), ("x", "z", "y", "hd"))
    cp = ("x", "z", "y")
    return jax.shard_map(
        local,
        mesh=inner,
        in_specs=(P(cp, "hd"), P(cp, "hd"), P(cp, "hd"), P(), P(), P("hd", None)),
        out_specs=P(cp + ("hd",), None),
        check_vma=False,
    )
```

```python
import jax
import jax.numpy as jnp
from jax import lax
from jax.experimental import pallas as pl
from jax.experimental.pallas import tpu as pltpu
from jax.sharding import Mesh, PartitionSpec as P

HEAD = 128
SPAN = 96
RING = 4
GROUP = 4
ROWS = GROUP * SPAN
DOCS = 8
LOW = -1e30
LOG2E = 1.4426950408889634
FACTOR = HEAD ** -0.5 * LOG2E
MAX_TASKS = 160

PHASES = (((0, 0), (0, 1)), ((1, 0), (1, 1), (3, 0), (3, 1)), ((2, 0), (2, 1)))
CHUNKS = (256, 512, 256)


def shift(value, axis, by):
    return lax.ppermute(value, axis, [(i, (i + by) % RING) for i in range(RING)])


def phase_kernel(phase, *refs):
    chunk = CHUNKS[phase]
    first_phase, last_phase = phase == 0, phase == 2
    order = PHASES[phase]
    refs = list(refs)

    def take(n):
        out = refs[:n]
        del refs[:n]
        return out

    coords, table, starts, rank = take(4)
    pieces = take(2 * len(order))
    if first_phase:
        q_parts = take(4)
        q_all, best_all, acc_all = take(3)
    else:
        q_all, best_in, acc_in = take(3)
        if last_phase:
            outs = take(4)
            best_all, acc_all = take(2)
        else:
            (weight,) = take(1)
            best_all, acc_all, weight_held = take(3)
            weight_copy = pltpu.make_async_copy(weight, weight_held, refs.pop())
            weight_copy.start()
    kv, low_all, high_all, s0, s1, task_span, task_first, task_upper, sem = refs
    x, z, y = coords[0], coords[1], coords[2]

    def slot_of(dx, dz, dy, half):
        cp = ((x + RING - dx) % RING) * 16 + ((z + RING - dz) % RING) * 4 + (y + RING - dy) % RING
        return 2 * cp + half

    for family in range(2):
        for index, (far, upper_block) in enumerate(order):
            ref = pieces[family * len(order) + index]
            for i in range(8):
                near = 2 * upper_block + i // 4
                dy = 2 * family + (i // 2) % 2
                dx, dz = (far, near) if family == 0 else (near, far)
                row = rank[table[slot_of(dx, dz, dy, i % 2)]] * SPAN
                pltpu.make_async_copy(
                    ref.at[pl.ds(i * SPAN, SPAN)], kv.at[pl.ds(pl.multiple_of(row, SPAN), SPAN)], sem
                ).start()

    if first_phase:
        for s, ref in enumerate(q_parts):
            for half in range(2):
                for h in range(GROUP):
                    q_all[2 * s + half, h * SPAN : (h + 1) * SPAN, :] = ref[
                        half * SPAN : (half + 1) * SPAN, h * HEAD : (h + 1) * HEAD
                    ]
        best_all[...] = jnp.full(best_all.shape, LOW, jnp.float32)
        acc_all[...] = jnp.zeros(acc_all.shape, jnp.float32)
    else:
        best_all[...] = best_in[...]
        acc_all[...] = acc_in[...]

    doc_low = []
    for d in range(DOCS):
        span = starts[d] // SPAN
        doc_low.append(rank[span] * SPAN + (rank[span + 1] - rank[span]) * (starts[d] - span * SPAN))

    def plan(i, total):
        span = table[slot_of(0, 0, i // 2, i % 2)]
        row = lax.broadcasted_iota(jnp.int32, (SPAN, HEAD), 0)
        low = jnp.full((SPAN, HEAD), doc_low[0], jnp.int32)
        low_min = doc_low[0]
        for d in range(1, DOCS):
            low = jnp.where(row >= starts[d] - span * SPAN, doc_low[d], low)
            low_min = jnp.where(starts[d] <= span * SPAN, doc_low[d], low_min)
        low_all[i] = low
        base, top = rank[span] * SPAN, rank[span + 1] * SPAN
        high_all[i] = jnp.where(top > base, base + row, base - 1)

        def add(e, n):
            task_span[n] = i
            task_upper[n] = top - e * chunk
            task_first[n] = jnp.maximum(top - (e + 1) * chunk, 0)
            return n + 1

        return lax.fori_loop(0, (top - low_min + chunk - 1) // chunk, add, total)

    total = lax.fori_loop(0, 8, plan, 0)
    for extra in range(3):
        task_span[total + extra] = 0
        task_first[total + extra] = 0
        task_upper[total + extra] = 0

    pltpu.make_async_copy(kv, kv, sem).wait()
    ones = jnp.ones((chunk, HEAD), jnp.bfloat16)
    lanes = chunk // HEAD

    def score(t, out):
        k = kv[pl.ds(pl.multiple_of(task_first[t], 32), chunk), :HEAD]
        out[...] = lax.dot_general(
            q_all[task_span[t]], k, (((1,), (1,)), ((), ())), preferred_element_type=jnp.float32
        )

    def absorb(t, s_ref):
        i, k0 = task_span[t], pl.multiple_of(task_first[t], 32)
        low = low_all[i] - k0
        high = jnp.minimum(high_all[i], task_upper[t] - 1) - k0
        lane = lax.broadcasted_iota(jnp.int32, (SPAN, HEAD), 1)
        seen = [(lane >= low - g * HEAD) & (lane <= high - g * HEAD) for g in range(lanes)]
        weights, fades = [], []
        for h in range(GROUP):
            at = slice(h * SPAN, (h + 1) * SPAN)
            s = [
                jnp.where(seen[g], s_ref[at, g * HEAD : (g + 1) * HEAD], 2 * LOW) for g in range(lanes)
            ]
            top = s[0]
            for g in range(1, lanes):
                top = jnp.maximum(top, s[g])
            best = best_all[i, at, :]
            new_best = jnp.maximum(best, jnp.max(top, axis=1, keepdims=True))
            best_all[i, at, :] = new_best
            fades.append(jnp.exp2((best - new_best) * FACTOR))
            weights.append(
                jnp.concatenate(
                    [jnp.exp2((part - new_best) * FACTOR).astype(jnp.bfloat16) for part in s], axis=1
                )
            )
        v = jnp.concatenate([kv[pl.ds(k0, chunk), HEAD:], ones], axis=1)
        part = jnp.dot(jnp.concatenate(weights, axis=0), v, preferred_element_type=jnp.float32)
        for h in range(GROUP):
            at = slice(h * SPAN, (h + 1) * SPAN)
            for half in range(2):
                cols = slice(half * HEAD, (half + 1) * HEAD)
                acc_all[i, at, cols] = acc_all[i, at, cols] * fades[h] + part[at, cols]

    score(0, s0)

    def pair(j, _):
        t = 2 * j
        score(t + 1, s1)
        absorb(t, s0)
        score(t + 2, s0)
        absorb(t + 1, s1)
        return 0

    lax.fori_loop(0, (total + 1) // 2, pair, 0)

    if phase == 1:
        weight_copy.wait()
    if last_phase:
        for s, ref in enumerate(outs):
            for half in range(2):
                for h in range(GROUP):
                    at = slice(h * SPAN, (h + 1) * SPAN)
                    i = 2 * s + half
                    ref[half * SPAN : (half + 1) * SPAN, h * HEAD : (h + 1) * HEAD] = (
                        acc_all[i, at, :HEAD] / acc_all[i, at, HEAD:]
                    ).astype(jnp.bfloat16)


def run_phase(phase, scalars, pieces, others, weight=None):
    smem = pl.BlockSpec(memory_space=pltpu.SMEM)
    vmem = pl.BlockSpec(memory_space=pltpu.VMEM)
    hbm = pl.BlockSpec(memory_space=pl.ANY)
    chunk = CHUNKS[phase]
    keys = sum(piece.shape[0] for piece in pieces)
    state = [((8, ROWS, HEAD), jnp.float32), ((8, ROWS, 2 * HEAD), jnp.float32)]
    if phase == 0:
        outs = [((8, ROWS, HEAD), jnp.bfloat16)] + state
    elif phase == 1:
        outs = state + [(weight.shape, jnp.bfloat16)]
    else:
        outs = [((2 * SPAN, GROUP * HEAD), jnp.bfloat16)] * 4
    scratch = [pltpu.VMEM(*s) for s in state] if phase == 2 else []
    scratch += [
        pltpu.VMEM((keys, 2 * HEAD), jnp.bfloat16),
        pltpu.VMEM((8, SPAN, HEAD), jnp.int32),
        pltpu.VMEM((8, SPAN, HEAD), jnp.int32),
        pltpu.VMEM((ROWS, chunk), jnp.float32),
        pltpu.VMEM((ROWS, chunk), jnp.float32),
        pltpu.SMEM((MAX_TASKS,), jnp.int32),
        pltpu.SMEM((MAX_TASKS,), jnp.int32),
        pltpu.SMEM((MAX_TASKS,), jnp.int32),
        pltpu.SemaphoreType.DMA,
    ]
    far = [] if weight is None else [weight]
    scratch += [pltpu.SemaphoreType.DMA] * len(far)
    share = len(pieces) / 16
    return pl.pallas_call(
        lambda *refs: phase_kernel(phase, *refs),
        out_shape=[jax.ShapeDtypeStruct(*o) for o in outs],
        in_specs=[smem] * 4 + [hbm] * len(pieces) + [vmem] * len(others) + [pl.BlockSpec(memory_space=pltpu.HBM)] * len(far),
        out_specs=[vmem] * len(outs),
        scratch_shapes=scratch,
        compiler_params=pltpu.CompilerParams(vmem_limit_bytes=16 * 1024 * 1024),
        cost_estimate=pl.CostEstimate(
            flops=int(8e9 * share), bytes_accessed=int(1e7 * share), transcendentals=int(1e7 * share)
        ),
        name=f"attention_{phase}",
    )(*scalars, *pieces, *others, *far)


def project_kernel(first, coords, o0, o1, o2, o3, w, keep, send, scr):
    y, core = coords[2], coords[3]
    block = scr.shape[1]
    for n in range(keep.shape[1] // block):
        cols = slice(first + n * block, first + (n + 1) * block)
        acc = None
        for s, ref in enumerate((o0, o1, o2, o3)):
            row = pl.multiple_of(((y + s) % RING) * 512, 512)
            part = jnp.dot(ref[...], w[pl.ds(row, 512), cols], preferred_element_type=jnp.float32)
            acc = part if acc is None else acc + part
        scr[...] = acc
        at = slice(n * block, (n + 1) * block)
        keep[:, at] = scr[pl.ds(pl.multiple_of(core * SPAN, SPAN), SPAN), :]
        send[:, at] = scr[pl.ds(pl.multiple_of((1 - core) * SPAN, SPAN), SPAN), :].astype(jnp.bfloat16)


def project(coords, o_parts, weight, first, width):
    smem = pl.BlockSpec(memory_space=pltpu.SMEM)
    vmem = pl.BlockSpec(memory_space=pltpu.VMEM)
    return pl.pallas_call(
        lambda *refs: project_kernel(first, *refs),
        out_shape=[
            jax.ShapeDtypeStruct((SPAN, width), jnp.float32),
            jax.ShapeDtypeStruct((SPAN, width), jnp.bfloat16),
        ],
        in_specs=[smem] + [vmem] * 5,
        out_specs=[vmem, vmem],
        scratch_shapes=[pltpu.VMEM((2 * SPAN, 512), jnp.float32)],
        compiler_params=pltpu.CompilerParams(vmem_limit_bytes=16 * 1024 * 1024),
        cost_estimate=pl.CostEstimate(
            flops=2 * 192 * 2048 * width, bytes_accessed=2048 * width * 2, transcendentals=0
        ),
        name="project",
    )(coords, *o_parts, weight)


def local(queries, keys, values, span_table, doc_ids, out_weight):
    rows = queries.shape[0]
    spans = span_table.shape[0]
    x, z, y, core = (lax.axis_index(a) for a in ("x", "z", "y", "hd"))
    coords = jnp.stack([x, z, y, core]).astype(jnp.int32)
    kv = jnp.concatenate([keys.reshape(rows, RING, HEAD), values.reshape(rows, RING, HEAD)], axis=2)
    kv = kv.transpose(1, 0, 2)
    part = [lax.dynamic_index_in_dim(kv, (y + s) % RING, 0, keepdims=False) for s in range(RING)]
    part = [part[0]] + [shift(part[s], "y", s) for s in range(1, RING)]
    low, high = jnp.concatenate(part[:2], 0), jnp.concatenate(part[2:], 0)

    q_part = [
        lax.dynamic_slice_in_dim(queries, ((y + s) % RING) * 512, 512, 1) for s in range(RING)
    ]
    q_part = [q_part[0]] + [shift(q_part[s], "y", s) for s in range(1, RING)]

    def gathered(block, near_axis, far_axis):
        near = [block] + [shift(block, near_axis, s) for s in range(1, RING)]
        first, second = jnp.concatenate(near[:2], 0), jnp.concatenate(near[2:], 0)
        ahead_first = shift(first, far_axis, 1)
        behind_second = shift(second, far_axis, -1)
        ahead_second = shift(second, far_axis, 1)
        behind_first = shift(first, far_axis, -1)
        far_first = shift(ahead_first, far_axis, 1)
        far_second = shift(behind_second, far_axis, -1)
        return [first, second], [ahead_first, ahead_second, behind_first, behind_second], [far_first, far_second]

    pieces = [a + b for a, b in zip(gathered(low, "z", "x"), gathered(high, "x", "z"))]

    docs = jnp.arange(DOCS, dtype=jnp.int32)
    starts = jnp.sum((doc_ids[None, :] < docs[:, None]).astype(jnp.int32), axis=1)
    slot = jnp.arange(spans, dtype=jnp.int32)
    cp = slot // 2
    dx, dz, dy = (x - cp // 16) % RING, (z - (cp // 4) % 4) % RING, (y - cp % 4) % RING
    far = jnp.where(dy < 2, dx, dz)
    phase_of = jnp.where(far == 0, 0, jnp.where(far == 2, 2, 1))
    before = span_table[None, :] < jnp.arange(spans + 8, dtype=jnp.int32)[:, None]
    ranks = [jnp.sum((before & (phase_of == p)[None, :]).astype(jnp.int32), axis=1) for p in range(3)]

    scalars = [coords, span_table, starts]
    q_all, best, acc = run_phase(0, scalars + [ranks[0]], pieces[0], q_part)
    best, acc, weight = run_phase(1, scalars + [ranks[1]], pieces[1], [q_all, best, acc], out_weight)
    o_part = run_phase(2, scalars + [ranks[2]], pieces[2], [q_all, best, acc])
    o_part = [o_part[0]] + [shift(o_part[s], "y", -s) for s in range(1, RING)]

    mixed = []
    width = out_weight.shape[1] // 2
    for n in range(2):
        keep, send = project(coords, o_part, weight, n * width, width)
        arrived = lax.ppermute(send, "hd", [(0, 1), (1, 0)])
        mixed.append((keep + arrived.astype(jnp.float32)).astype(jnp.bfloat16))
    return jnp.concatenate(mixed, axis=1)


def solution(mesh):
    inner = Mesh(mesh.devices.reshape(RING, RING, RING, 2), ("x", "z", "y", "hd"))
    cp = ("x", "z", "y")
    return jax.shard_map(
        local,
        mesh=inner,
        in_specs=(P(cp, "hd"), P(cp, "hd"), P(cp, "hd"), P(), P(), P("hd", None)),
        out_specs=P(cp + ("hd",), None),
        check_vma=False,
    )
```

```python
import jax
import jax.numpy as jnp
from jax import lax
from jax.experimental import pallas as pl
from jax.experimental.pallas import tpu as pltpu
from jax.sharding import Mesh, PartitionSpec as P

HEAD = 128
SPAN = 96
RING = 4
GROUP = 4
ROWS = GROUP * SPAN
DOCS = 8
LOW = -1e30
LOG2E = 1.4426950408889634
FACTOR = HEAD ** -0.5 * LOG2E
MAX_TASKS = 160

PHASES = (((0, 0), (0, 1)), ((1, 0), (1, 1), (3, 0), (3, 1)), ((2, 0), (2, 1)))
CHUNKS = (256, 512, 256)


def shift(value, axis, by):
    return lax.ppermute(value, axis, [(i, (i + by) % RING) for i in range(RING)])


def phase_kernel(phase, *refs):
    chunk = CHUNKS[phase]
    first_phase, last_phase = phase == 0, phase == 2
    order = PHASES[phase]
    refs = list(refs)

    def take(n):
        out = refs[:n]
        del refs[:n]
        return out

    coords, table, starts, rank = take(4)
    pieces = take(2 * len(order))
    if first_phase:
        q_parts = take(4)
    else:
        (q_all,) = take(1)
        take(2)
    if phase == 1:
        (weight,) = take(1)
    if first_phase:
        (q_all,) = take(1)
    best_all, acc_all = take(2)
    if last_phase:
        outs = take(8)
    if phase == 1:
        (weight_held,) = take(1)
        weight_copy = pltpu.make_async_copy(weight, weight_held, refs.pop())
        weight_copy.start()
    kv, low_all, high_all, s0, s1, p0, p1, f0, f1, task_span, task_first, task_upper = refs
    x, z, y, core = coords[0], coords[1], coords[2], coords[3]

    def slot_of(dx, dz, dy, half):
        cp = ((x + RING - dx) % RING) * 16 + ((z + RING - dz) % RING) * 4 + (y + RING - dy) % RING
        return 2 * cp + half

    for family in range(2):
        for index, (far, upper_block) in enumerate(order):
            ref = pieces[family * len(order) + index]
            for i in range(8):
                near = 2 * upper_block + i // 4
                dy = 2 * family + (i // 2) % 2
                dx, dz = (far, near) if family == 0 else (near, far)
                row = rank[table[slot_of(dx, dz, dy, i % 2)]] * SPAN
                kv[pl.ds(pl.multiple_of(row, SPAN), SPAN), :] = ref[i * SPAN : (i + 1) * SPAN, :]

    if first_phase:
        for s, ref in enumerate(q_parts):
            for half in range(2):
                for h in range(GROUP):
                    q_all[2 * s + half, h * SPAN : (h + 1) * SPAN, :] = ref[
                        half * SPAN : (half + 1) * SPAN, h * HEAD : (h + 1) * HEAD
                    ]
        best_all[...] = jnp.full(best_all.shape, LOW, jnp.float32)
        acc_all[...] = jnp.zeros(acc_all.shape, jnp.float32)

    doc_low = []
    for d in range(DOCS):
        span = starts[d] // SPAN
        doc_low.append(rank[span] * SPAN + (rank[span + 1] - rank[span]) * (starts[d] - span * SPAN))

    def plan(i, total):
        span = table[slot_of(0, 0, i // 2, i % 2)]
        row = lax.broadcasted_iota(jnp.int32, (SPAN, HEAD), 0)
        low = jnp.full((SPAN, HEAD), doc_low[0], jnp.int32)
        low_min = doc_low[0]
        for d in range(1, DOCS):
            low = jnp.where(row >= starts[d] - span * SPAN, doc_low[d], low)
            low_min = jnp.where(starts[d] <= span * SPAN, doc_low[d], low_min)
        low_all[i] = low
        base, top = rank[span] * SPAN, rank[span + 1] * SPAN
        high_all[i] = jnp.where(top > base, base + row, base - 1)

        def add(e, n):
            task_span[n] = i
            task_upper[n] = top - e * chunk
            task_first[n] = jnp.maximum(top - (e + 1) * chunk, 0)
            return n + 1

        return lax.fori_loop(0, (top - low_min + chunk - 1) // chunk, add, total)

    total = lax.fori_loop(0, 8, plan, 1)
    task_span[0] = 0
    task_first[0] = 0
    for extra in range(3):
        task_span[total + extra] = 0
        task_first[total + extra] = 0
        task_upper[total + extra] = 0

    p1[...] = jnp.zeros(p1.shape, jnp.bfloat16)
    f1[...] = jnp.ones(f1.shape, jnp.float32)
    ones = jnp.ones((chunk, HEAD), jnp.bfloat16)
    lanes = chunk // HEAD

    def score(t, out):
        k = kv[pl.ds(pl.multiple_of(task_first[t], 32), chunk), :HEAD]
        out[...] = lax.dot_general(
            q_all[task_span[t]], k, (((1,), (1,)), ((), ())), preferred_element_type=jnp.float32
        )

    def weigh(t, s_ref, p_ref, f_ref):
        i, k0 = task_span[t], task_first[t]
        low = low_all[i] - k0
        high = jnp.minimum(high_all[i], task_upper[t] - 1) - k0
        lane = lax.broadcasted_iota(jnp.int32, (SPAN, HEAD), 1)
        seen = [(lane >= low - g * HEAD) & (lane <= high - g * HEAD) for g in range(lanes)]
        for h in range(GROUP):
            at = slice(h * SPAN, (h + 1) * SPAN)
            s = [
                jnp.where(seen[g], s_ref[at, g * HEAD : (g + 1) * HEAD], 2 * LOW) for g in range(lanes)
            ]
            top = s[0]
            for g in range(1, lanes):
                top = jnp.maximum(top, s[g])
            best = best_all[i, at, :]
            new_best = jnp.maximum(best, jnp.max(top, axis=1, keepdims=True))
            best_all[i, at, :] = new_best
            f_ref[at, :] = jnp.exp2((best - new_best) * FACTOR)
            for g in range(lanes):
                p_ref[at, g * HEAD : (g + 1) * HEAD] = jnp.exp2((s[g] - new_best) * FACTOR).astype(
                    jnp.bfloat16
                )

    def accumulate(t, p_ref, f_ref):
        i, k0 = task_span[t], pl.multiple_of(task_first[t], 32)
        v = jnp.concatenate([kv[pl.ds(k0, chunk), HEAD:], ones], axis=1)
        part = jnp.dot(p_ref[...], v, preferred_element_type=jnp.float32)
        fade = f_ref[...]
        for half in range(2):
            cols = slice(half * HEAD, (half + 1) * HEAD)
            acc_all[i, :, cols] = acc_all[i, :, cols] * fade + part[:, cols]

    score(1, s0)

    def pair(j, _):
        t = 2 * j + 1
        accumulate(t - 1, p1, f1)
        score(t + 1, s1)
        weigh(t, s0, p0, f0)
        accumulate(t, p0, f0)
        score(t + 2, s0)
        weigh(t + 1, s1, p1, f1)
        return 0

    pairs = total // 2
    lax.fori_loop(0, pairs, pair, 0)
    accumulate(2 * pairs, p1, f1)

    if phase == 1:
        weight_copy.wait()
    if last_phase:
        for turn in range(2):
            half = 1 - core if turn == 0 else core
            for s in range(RING):
                i = 2 * s + half
                for h in range(GROUP):
                    at = slice(h * SPAN, (h + 1) * SPAN)
                    outs[4 * turn + s][:, h * HEAD : (h + 1) * HEAD] = (
                        acc_all[i, at, :HEAD] / acc_all[i, at, HEAD:]
                    ).astype(jnp.bfloat16)


def run_phase(phase, scalars, pieces, others, weight=None):
    smem = pl.BlockSpec(memory_space=pltpu.SMEM)
    vmem = pl.BlockSpec(memory_space=pltpu.VMEM)
    chunk = CHUNKS[phase]
    keys = sum(piece.shape[0] for piece in pieces)
    state = [((8, ROWS, HEAD), jnp.float32), ((8, ROWS, 2 * HEAD), jnp.float32)]
    far = [] if weight is None else [weight]
    held = [(w.shape, w.dtype) for w in far]
    if phase == 0:
        outs = [((8, ROWS, HEAD), jnp.bfloat16)] + state + held
        aliases = {}
    else:
        outs = state + held
        first = 4 + len(pieces) + 1
        aliases = {first: 0, first + 1: 1}
    if phase == 2:
        outs = outs + [((SPAN, GROUP * HEAD), jnp.bfloat16)] * 8
    scratch = [
        pltpu.VMEM((keys, 2 * HEAD), jnp.bfloat16),
        pltpu.VMEM((8, SPAN, HEAD), jnp.int32),
        pltpu.VMEM((8, SPAN, HEAD), jnp.int32),
        pltpu.VMEM((ROWS, chunk), jnp.float32),
        pltpu.VMEM((ROWS, chunk), jnp.float32),
        pltpu.VMEM((ROWS, chunk), jnp.bfloat16),
        pltpu.VMEM((ROWS, chunk), jnp.bfloat16),
        pltpu.VMEM((ROWS, HEAD), jnp.float32),
        pltpu.VMEM((ROWS, HEAD), jnp.float32),
        pltpu.SMEM((MAX_TASKS,), jnp.int32),
        pltpu.SMEM((MAX_TASKS,), jnp.int32),
        pltpu.SMEM((MAX_TASKS,), jnp.int32),
    ] + [pltpu.SemaphoreType.DMA] * len(far)
    share = len(pieces) / 16
    return pl.pallas_call(
        lambda *refs: phase_kernel(phase, *refs),
        out_shape=[jax.ShapeDtypeStruct(*o) for o in outs],
        in_specs=[smem] * 4
        + [vmem] * (len(pieces) + len(others))
        + [pl.BlockSpec(memory_space=pltpu.HBM)] * len(far),
        out_specs=[vmem] * len(outs),
        scratch_shapes=scratch,
        input_output_aliases=aliases,
        compiler_params=pltpu.CompilerParams(vmem_limit_bytes=16 * 1024 * 1024),
        cost_estimate=pl.CostEstimate(
            flops=int(8e9 * share), bytes_accessed=int(1e7 * share), transcendentals=int(1e7 * share)
        ),
    )(*scalars, *pieces, *others, *far)


def project_kernel(coords, o0, o1, o2, o3, w, out):
    y = coords[2]
    block = 512
    for n in range(w.shape[1] // block):
        cols = slice(n * block, (n + 1) * block)
        acc = None
        for s, ref in enumerate((o0, o1, o2, o3)):
            row = pl.multiple_of(((y + s) % RING) * 512, 512)
            part = jnp.dot(ref[...], w[pl.ds(row, 512), cols], preferred_element_type=jnp.float32)
            acc = part if acc is None else acc + part
        out[:, cols] = acc.astype(out.dtype)


def project(coords, o_parts, weight, dtype):
    smem = pl.BlockSpec(memory_space=pltpu.SMEM)
    vmem = pl.BlockSpec(memory_space=pltpu.VMEM)
    width = weight.shape[1]
    return pl.pallas_call(
        project_kernel,
        out_shape=jax.ShapeDtypeStruct((SPAN, width), dtype),
        in_specs=[smem] + [vmem] * 5,
        out_specs=vmem,
        compiler_params=pltpu.CompilerParams(vmem_limit_bytes=16 * 1024 * 1024),
        cost_estimate=pl.CostEstimate(
            flops=2 * SPAN * 2048 * width, bytes_accessed=2048 * width * 2, transcendentals=0
        ),
        name="project",
    )(coords, *o_parts, weight)


def layer(queries, keys, values, span_table, doc_ids, out_weight):
    rows = queries.shape[0]
    spans = span_table.shape[0]
    x, z, y, core = (lax.axis_index(a) for a in ("x", "z", "y", "hd"))
    coords = jnp.stack([x, z, y, core]).astype(jnp.int32)
    kv = jnp.concatenate([keys.reshape(rows, RING, HEAD), values.reshape(rows, RING, HEAD)], axis=2)
    kv = kv.transpose(1, 0, 2)
    part = [lax.dynamic_index_in_dim(kv, (y + s) % RING, 0, keepdims=False) for s in range(RING)]
    part = [part[0]] + [shift(part[s], "y", s) for s in range(1, RING)]
    low, high = jnp.concatenate(part[:2], 0), jnp.concatenate(part[2:], 0)

    q_part = [
        lax.dynamic_slice_in_dim(queries, ((y + s) % RING) * 512, 512, 1) for s in range(RING)
    ]
    q_part = [q_part[0]] + [shift(q_part[s], "y", s) for s in range(1, RING)]

    def gathered(block, near_axis, far_axis):
        near = [block] + [shift(block, near_axis, s) for s in range(1, RING)]
        first, second = jnp.concatenate(near[:2], 0), jnp.concatenate(near[2:], 0)
        ahead_first = shift(first, far_axis, 1)
        behind_second = shift(second, far_axis, -1)
        ahead_second = shift(second, far_axis, 1)
        behind_first = shift(first, far_axis, -1)
        far_first = shift(ahead_first, far_axis, 1)
        far_second = shift(behind_second, far_axis, -1)
        return [first, second], [ahead_first, ahead_second, behind_first, behind_second], [far_first, far_second]

    pieces = [a + b for a, b in zip(gathered(low, "z", "x"), gathered(high, "x", "z"))]

    docs = jnp.arange(DOCS, dtype=jnp.int32)
    starts = jnp.sum((doc_ids[None, :] < docs[:, None]).astype(jnp.int32), axis=1)
    slot = jnp.arange(spans, dtype=jnp.int32)
    cp = slot // 2
    dx, dz, dy = (x - cp // 16) % RING, (z - (cp // 4) % 4) % RING, (y - cp % 4) % RING
    far = jnp.where(dy < 2, dx, dz)
    phase_of = jnp.where(far == 0, 0, jnp.where(far == 2, 2, 1))
    before = span_table[None, :] < jnp.arange(spans + 8, dtype=jnp.int32)[:, None]
    ranks = [jnp.sum((before & (phase_of == p)[None, :]).astype(jnp.int32), axis=1) for p in range(3)]

    scalars = [coords, span_table, starts]
    q_all, best, acc = run_phase(0, scalars + [ranks[0]], pieces[0], q_part)
    best, acc, weight = run_phase(1, scalars + [ranks[1]], pieces[1], [q_all, best, acc], out_weight)
    o_part = run_phase(2, scalars + [ranks[2]], pieces[2], [q_all, best, acc])[2:]

    def returned(part):
        return [part[0]] + [shift(part[s], "y", -s) for s in range(1, RING)]

    theirs, ours = returned(o_part[:4]), returned(o_part[4:])
    sent = lax.ppermute(project(coords, theirs, weight, jnp.bfloat16), "hd", [(0, 1), (1, 0)])
    kept = project(coords, ours, weight, jnp.float32)
    return (kept + sent.astype(jnp.float32)).astype(jnp.bfloat16)


def solution(mesh):
    inner = Mesh(mesh.devices.reshape(RING, RING, RING, 2), ("x", "z", "y", "hd"))
    cp = ("x", "z", "y")
    return jax.shard_map(
        layer,
        mesh=inner,
        in_specs=(P(cp, "hd"), P(cp, "hd"), P(cp, "hd"), P(), P(), P("hd", None)),
        out_specs=P(cp + ("hd",), None),
        check_vma=False,
    )
```

```python
import jax
import jax.numpy as jnp
from jax import lax
from jax.experimental import pallas as pl
from jax.experimental.pallas import tpu as pltpu
from jax.sharding import Mesh, PartitionSpec as P

HEAD = 128
SPAN = 96
RING = 4
GROUP = 4
ROWS = GROUP * SPAN
DOCS = 8
LOW = -1e30
LOG2E = 1.4426950408889634
FACTOR = HEAD ** -0.5 * LOG2E
MAX_TASKS = 160

PHASES = (((0, 0), (0, 1)), ((1, 0), (3, 1)), ((1, 1), (3, 0)), ((2, 0), (2, 1)))
CHUNKS = (256, 256, 256, 256)


def shift(value, axis, by):
    return lax.ppermute(value, axis, [(i, (i + by) % RING) for i in range(RING)])


def phase_kernel(phase, *refs):
    chunk = CHUNKS[phase]
    first_phase, last_phase = phase == 0, phase == 3
    order = PHASES[phase]
    refs = list(refs)

    def take(n):
        out = refs[:n]
        del refs[:n]
        return out

    coords, table, starts, rank = take(4)
    pieces = take(2 * len(order))
    if first_phase:
        q_parts = take(4)
    else:
        (q_all,) = take(1)
        take(2)
    if phase == 1:
        (weight,) = take(1)
    if first_phase:
        (q_all,) = take(1)
    best_all, acc_all = take(2)
    if last_phase:
        outs = take(8)
    if phase == 1:
        (weight_held,) = take(1)
        weight_copy = pltpu.make_async_copy(weight, weight_held, refs.pop())
        weight_copy.start()
    kv, low_all, high_all, s0, s1, p0, p1, f0, f1, task_span, task_first, task_upper = refs
    x, z, y, core = coords[0], coords[1], coords[2], coords[3]

    def slot_of(dx, dz, dy, half):
        cp = ((x + RING - dx) % RING) * 16 + ((z + RING - dz) % RING) * 4 + (y + RING - dy) % RING
        return 2 * cp + half

    for family in range(2):
        for index, (far, upper_block) in enumerate(order):
            ref = pieces[family * len(order) + index]
            for i in range(8):
                near = 2 * upper_block + i // 4
                dy = 2 * family + (i // 2) % 2
                dx, dz = (far, near) if family == 0 else (near, far)
                row = rank[table[slot_of(dx, dz, dy, i % 2)]] * SPAN
                kv[pl.ds(pl.multiple_of(row, SPAN), SPAN), :] = ref[i * SPAN : (i + 1) * SPAN, :]

    if first_phase:
        for s, ref in enumerate(q_parts):
            for half in range(2):
                for h in range(GROUP):
                    q_all[2 * s + half, h * SPAN : (h + 1) * SPAN, :] = ref[
                        half * SPAN : (half + 1) * SPAN, h * HEAD : (h + 1) * HEAD
                    ]
        best_all[...] = jnp.full(best_all.shape, LOW, jnp.float32)
        acc_all[...] = jnp.zeros(acc_all.shape, jnp.float32)

    doc_low = []
    for d in range(DOCS):
        span = starts[d] // SPAN
        doc_low.append(rank[span] * SPAN + (rank[span + 1] - rank[span]) * (starts[d] - span * SPAN))

    def plan(i, total):
        span = table[slot_of(0, 0, i // 2, i % 2)]
        row = lax.broadcasted_iota(jnp.int32, (SPAN, HEAD), 0)
        low = jnp.full((SPAN, HEAD), doc_low[0], jnp.int32)
        low_min = doc_low[0]
        for d in range(1, DOCS):
            low = jnp.where(row >= starts[d] - span * SPAN, doc_low[d], low)
            low_min = jnp.where(starts[d] <= span * SPAN, doc_low[d], low_min)
        low_all[i] = low
        base, top = rank[span] * SPAN, rank[span + 1] * SPAN
        high_all[i] = jnp.where(top > base, base + row, base - 1)

        def add(e, n):
            task_span[n] = i
            task_upper[n] = top - e * chunk
            task_first[n] = jnp.maximum(top - (e + 1) * chunk, 0)
            return n + 1

        return lax.fori_loop(0, (top - low_min + chunk - 1) // chunk, add, total)

    total = lax.fori_loop(0, 8, plan, 1)
    task_span[0] = 0
    task_first[0] = 0
    for extra in range(3):
        task_span[total + extra] = 0
        task_first[total + extra] = 0
        task_upper[total + extra] = 0

    p1[...] = jnp.zeros(p1.shape, jnp.bfloat16)
    f1[...] = jnp.ones(f1.shape, jnp.float32)
    ones = jnp.ones((chunk, HEAD), jnp.bfloat16)
    lanes = chunk // HEAD

    def score(t, out):
        k = kv[pl.ds(pl.multiple_of(task_first[t], 32), chunk), :HEAD]
        out[...] = lax.dot_general(
            q_all[task_span[t]], k, (((1,), (1,)), ((), ())), preferred_element_type=jnp.float32
        )

    def weigh(t, s_ref, p_ref, f_ref):
        i, k0 = task_span[t], task_first[t]
        low = low_all[i] - k0
        high = jnp.minimum(high_all[i], task_upper[t] - 1) - k0
        lane = lax.broadcasted_iota(jnp.int32, (SPAN, HEAD), 1)
        seen = [(lane >= low - g * HEAD) & (lane <= high - g * HEAD) for g in range(lanes)]
        for h in range(GROUP):
            at = slice(h * SPAN, (h + 1) * SPAN)
            s = [
                jnp.where(seen[g], s_ref[at, g * HEAD : (g + 1) * HEAD], 2 * LOW) for g in range(lanes)
            ]
            top = s[0]
            for g in range(1, lanes):
                top = jnp.maximum(top, s[g])
            best = best_all[i, at, :]
            new_best = jnp.maximum(best, jnp.max(top, axis=1, keepdims=True))
            best_all[i, at, :] = new_best
            f_ref[at, :] = jnp.exp2((best - new_best) * FACTOR)
            for g in range(lanes):
                p_ref[at, g * HEAD : (g + 1) * HEAD] = jnp.exp2((s[g] - new_best) * FACTOR).astype(
                    jnp.bfloat16
                )

    def accumulate(t, p_ref, f_ref):
        i, k0 = task_span[t], pl.multiple_of(task_first[t], 32)
        v = jnp.concatenate([kv[pl.ds(k0, chunk), HEAD:], ones], axis=1)
        part = jnp.dot(p_ref[...], v, preferred_element_type=jnp.float32)
        fade = f_ref[...]
        for half in range(2):
            cols = slice(half * HEAD, (half + 1) * HEAD)
            acc_all[i, :, cols] = acc_all[i, :, cols] * fade + part[:, cols]

    score(1, s0)

    def pair(j, _):
        t = 2 * j + 1
        accumulate(t - 1, p1, f1)
        score(t + 1, s1)
        weigh(t, s0, p0, f0)
        accumulate(t, p0, f0)
        score(t + 2, s0)
        weigh(t + 1, s1, p1, f1)
        return 0

    pairs = total // 2
    lax.fori_loop(0, pairs, pair, 0)
    accumulate(2 * pairs, p1, f1)

    if phase == 1:
        weight_copy.wait()
    if last_phase:
        for turn in range(2):
            half = 1 - core if turn == 0 else core
            for s in range(RING):
                i = 2 * s + half
                for h in range(GROUP):
                    at = slice(h * SPAN, (h + 1) * SPAN)
                    outs[4 * turn + s][:, h * HEAD : (h + 1) * HEAD] = (
                        acc_all[i, at, :HEAD] / acc_all[i, at, HEAD:]
                    ).astype(jnp.bfloat16)


def run_phase(phase, scalars, pieces, others, weight=None):
    smem = pl.BlockSpec(memory_space=pltpu.SMEM)
    vmem = pl.BlockSpec(memory_space=pltpu.VMEM)
    chunk = CHUNKS[phase]
    keys = sum(piece.shape[0] for piece in pieces)
    state = [((8, ROWS, HEAD), jnp.float32), ((8, ROWS, 2 * HEAD), jnp.float32)]
    far = [] if weight is None else [weight]
    held = [(w.shape, w.dtype) for w in far]
    if phase == 0:
        outs = [((8, ROWS, HEAD), jnp.bfloat16)] + state + held
        aliases = {}
    else:
        outs = state + held
        first = 4 + len(pieces) + 1
        aliases = {first: 0, first + 1: 1}
    if phase == 3:
        outs = outs + [((SPAN, GROUP * HEAD), jnp.bfloat16)] * 8
    scratch = [
        pltpu.VMEM((keys, 2 * HEAD), jnp.bfloat16),
        pltpu.VMEM((8, SPAN, HEAD), jnp.int32),
        pltpu.VMEM((8, SPAN, HEAD), jnp.int32),
        pltpu.VMEM((ROWS, chunk), jnp.float32),
        pltpu.VMEM((ROWS, chunk), jnp.float32),
        pltpu.VMEM((ROWS, chunk), jnp.bfloat16),
        pltpu.VMEM((ROWS, chunk), jnp.bfloat16),
        pltpu.VMEM((ROWS, HEAD), jnp.float32),
        pltpu.VMEM((ROWS, HEAD), jnp.float32),
        pltpu.SMEM((MAX_TASKS,), jnp.int32),
        pltpu.SMEM((MAX_TASKS,), jnp.int32),
        pltpu.SMEM((MAX_TASKS,), jnp.int32),
    ] + [pltpu.SemaphoreType.DMA] * len(far)
    share = len(pieces) / 16
    return pl.pallas_call(
        lambda *refs: phase_kernel(phase, *refs),
        out_shape=[jax.ShapeDtypeStruct(*o) for o in outs],
        in_specs=[smem] * 4
        + [vmem] * (len(pieces) + len(others))
        + [pl.BlockSpec(memory_space=pltpu.HBM)] * len(far),
        out_specs=[vmem] * len(outs),
        scratch_shapes=scratch,
        input_output_aliases=aliases,
        compiler_params=pltpu.CompilerParams(vmem_limit_bytes=16 * 1024 * 1024),
        cost_estimate=pl.CostEstimate(
            flops=int(8e9 * share), bytes_accessed=int(1e7 * share), transcendentals=int(1e7 * share)
        ),
    )(*scalars, *pieces, *others, *far)


def project_kernel(coords, o0, o1, o2, o3, w, out):
    y = coords[2]
    block = 512
    for n in range(w.shape[1] // block):
        cols = slice(n * block, (n + 1) * block)
        acc = None
        for s, ref in enumerate((o0, o1, o2, o3)):
            row = pl.multiple_of(((y + s) % RING) * 512, 512)
            part = jnp.dot(ref[...], w[pl.ds(row, 512), cols], preferred_element_type=jnp.float32)
            acc = part if acc is None else acc + part
        out[:, cols] = acc.astype(out.dtype)


def project(coords, o_parts, weight, dtype):
    smem = pl.BlockSpec(memory_space=pltpu.SMEM)
    vmem = pl.BlockSpec(memory_space=pltpu.VMEM)
    width = weight.shape[1]
    return pl.pallas_call(
        project_kernel,
        out_shape=jax.ShapeDtypeStruct((SPAN, width), dtype),
        in_specs=[smem] + [vmem] * 5,
        out_specs=vmem,
        compiler_params=pltpu.CompilerParams(vmem_limit_bytes=16 * 1024 * 1024),
        cost_estimate=pl.CostEstimate(
            flops=2 * SPAN * 2048 * width, bytes_accessed=2048 * width * 2, transcendentals=0
        ),
        name="project",
    )(coords, *o_parts, weight)


def layer(queries, keys, values, span_table, doc_ids, out_weight):
    rows = queries.shape[0]
    spans = span_table.shape[0]
    x, z, y, core = (lax.axis_index(a) for a in ("x", "z", "y", "hd"))
    coords = jnp.stack([x, z, y, core]).astype(jnp.int32)
    kv = jnp.concatenate([keys.reshape(rows, RING, HEAD), values.reshape(rows, RING, HEAD)], axis=2)
    kv = kv.transpose(1, 0, 2)
    part = [lax.dynamic_index_in_dim(kv, (y + s) % RING, 0, keepdims=False) for s in range(RING)]
    part = [part[0]] + [shift(part[s], "y", s) for s in range(1, RING)]
    low, high = jnp.concatenate(part[:2], 0), jnp.concatenate(part[2:], 0)

    q_part = [
        lax.dynamic_slice_in_dim(queries, ((y + s) % RING) * 512, 512, 1) for s in range(RING)
    ]
    q_part = [q_part[0]] + [shift(q_part[s], "y", s) for s in range(1, RING)]

    def gathered(block, near_axis, far_axis):
        near = [block] + [shift(block, near_axis, s) for s in range(1, RING)]
        first, second = jnp.concatenate(near[:2], 0), jnp.concatenate(near[2:], 0)
        ahead_first = shift(first, far_axis, 1)
        behind_second = shift(second, far_axis, -1)
        ahead_second = shift(second, far_axis, 1)
        behind_first = shift(first, far_axis, -1)
        far_first = shift(ahead_first, far_axis, 1)
        far_second = shift(behind_second, far_axis, -1)
        return [first, second], [ahead_first, behind_second], [ahead_second, behind_first], [far_first, far_second]

    pieces = [a + b for a, b in zip(gathered(low, "z", "x"), gathered(high, "x", "z"))]

    docs = jnp.arange(DOCS, dtype=jnp.int32)
    starts = jnp.sum((doc_ids[None, :] < docs[:, None]).astype(jnp.int32), axis=1)
    slot = jnp.arange(spans, dtype=jnp.int32)
    cp = slot // 2
    dx, dz, dy = (x - cp // 16) % RING, (z - (cp // 4) % 4) % RING, (y - cp % 4) % RING
    far, near = jnp.where(dy < 2, dx, dz), jnp.where(dy < 2, dz, dx)
    early = (far == 1) == (near < 2)
    phase_of = jnp.where(far == 0, 0, jnp.where(far == 2, 3, jnp.where(early, 1, 2)))
    before = span_table[None, :] < jnp.arange(spans + 8, dtype=jnp.int32)[:, None]
    ranks = [jnp.sum((before & (phase_of == p)[None, :]).astype(jnp.int32), axis=1) for p in range(4)]

    scalars = [coords, span_table, starts]
    q_all, best, acc = run_phase(0, scalars + [ranks[0]], pieces[0], q_part)
    best, acc, weight = run_phase(1, scalars + [ranks[1]], pieces[1], [q_all, best, acc], out_weight)
    best, acc = run_phase(2, scalars + [ranks[2]], pieces[2], [q_all, best, acc])
    o_part = run_phase(3, scalars + [ranks[3]], pieces[3], [q_all, best, acc])[2:]

    def returned(part):
        return [part[0]] + [shift(part[s], "y", -s) for s in range(1, RING)]

    theirs, ours = returned(o_part[:4]), returned(o_part[4:])
    sent = lax.ppermute(project(coords, theirs, weight, jnp.bfloat16), "hd", [(0, 1), (1, 0)])
    kept = project(coords, ours, weight, jnp.float32)
    return (kept + sent.astype(jnp.float32)).astype(jnp.bfloat16)


def solution(mesh):
    inner = Mesh(mesh.devices.reshape(RING, RING, RING, 2), ("x", "z", "y", "hd"))
    cp = ("x", "z", "y")
    return jax.shard_map(
        layer,
        mesh=inner,
        in_specs=(P(cp, "hd"), P(cp, "hd"), P(cp, "hd"), P(), P(), P("hd", None)),
        out_specs=P(cp + ("hd",), None),
        check_vma=False,
    )
```

```python
import jax
import jax.numpy as jnp
from jax import lax
from jax.experimental import pallas as pl
from jax.experimental.pallas import tpu as pltpu
from jax.sharding import Mesh, PartitionSpec as P

HEAD = 128
SPAN = 96
RING = 4
GROUP = 4
ROWS = GROUP * SPAN
DOCS = 8
LOW = -1e30
LOG2E = 1.4426950408889634
FACTOR = HEAD ** -0.5 * LOG2E
MAX_TASKS = 160

PHASES = (((0, 0), (0, 1)), ((1, 0), (3, 1)), ((1, 1), (3, 0)), ((2, 0), (2, 1)))
CHUNKS = (256, 256, 256, 256)


def shift(value, axis, by):
    return lax.ppermute(value, axis, [(i, (i + by) % RING) for i in range(RING)])


def phase_kernel(phase, *refs):
    chunk = CHUNKS[phase]
    first_phase, last_phase = phase == 0, phase == 3
    order = PHASES[phase]
    refs = list(refs)

    def take(n):
        out = refs[:n]
        del refs[:n]
        return out

    coords, table, starts, rank = take(4)
    pieces = take(2 * len(order))
    if first_phase:
        q_parts = take(4)
    else:
        (q_all,) = take(1)
        take(2)
    if first_phase:
        (weight,) = take(1)
        (q_all,) = take(1)
    best_all, acc_all = take(2)
    if last_phase:
        outs = take(8)
    if first_phase:
        (weight_held,) = take(1)
        weight_copy = pltpu.make_async_copy(weight, weight_held, refs.pop())
        weight_copy.start()
    kv, low_all, high_all, s0, s1, p0, p1, f0, f1, task_span, task_first, task_upper = refs
    x, z, y, core = coords[0], coords[1], coords[2], coords[3]

    def slot_of(dx, dz, dy, half):
        cp = ((x + RING - dx) % RING) * 16 + ((z + RING - dz) % RING) * 4 + (y + RING - dy) % RING
        return 2 * cp + half

    for family in range(2):
        for index, (far, upper_block) in enumerate(order):
            ref = pieces[family * len(order) + index]
            for i in range(8):
                near = 2 * upper_block + i // 4
                dy = 2 * family + (i // 2) % 2
                dx, dz = (far, near) if family == 0 else (near, far)
                row = rank[table[slot_of(dx, dz, dy, i % 2)]] * SPAN
                kv[pl.ds(pl.multiple_of(row, SPAN), SPAN), :] = ref[i * SPAN : (i + 1) * SPAN, :]

    if first_phase:
        for s, ref in enumerate(q_parts):
            for half in range(2):
                for h in range(GROUP):
                    q_all[2 * s + half, h * SPAN : (h + 1) * SPAN, :] = ref[
                        half * SPAN : (half + 1) * SPAN, h * HEAD : (h + 1) * HEAD
                    ]
        best_all[...] = jnp.full(best_all.shape, LOW, jnp.float32)
        acc_all[...] = jnp.zeros(acc_all.shape, jnp.float32)

    doc_low = []
    for d in range(DOCS):
        span = starts[d] // SPAN
        doc_low.append(rank[span] * SPAN + (rank[span + 1] - rank[span]) * (starts[d] - span * SPAN))

    def plan(i, total):
        span = table[slot_of(0, 0, i // 2, i % 2)]
        row = lax.broadcasted_iota(jnp.int32, (SPAN, HEAD), 0)
        low = jnp.full((SPAN, HEAD), doc_low[0], jnp.int32)
        low_min = doc_low[0]
        for d in range(1, DOCS):
            low = jnp.where(row >= starts[d] - span * SPAN, doc_low[d], low)
            low_min = jnp.where(starts[d] <= span * SPAN, doc_low[d], low_min)
        low_all[i] = low
        base, top = rank[span] * SPAN, rank[span + 1] * SPAN
        high_all[i] = jnp.where(top > base, base + row, base - 1)

        def add(e, n):
            task_span[n] = i
            task_upper[n] = top - e * chunk
            task_first[n] = jnp.maximum(top - (e + 1) * chunk, 0)
            return n + 1

        return lax.fori_loop(0, (top - low_min + chunk - 1) // chunk, add, total)

    total = lax.fori_loop(0, 8, plan, 1)
    task_span[0] = 0
    task_first[0] = 0
    for extra in range(3):
        task_span[total + extra] = 0
        task_first[total + extra] = 0
        task_upper[total + extra] = 0

    p1[...] = jnp.zeros(p1.shape, jnp.bfloat16)
    f1[...] = jnp.ones(f1.shape, jnp.float32)
    ones = jnp.ones((chunk, HEAD), jnp.bfloat16)
    lanes = chunk // HEAD

    def score(t, out):
        k = kv[pl.ds(pl.multiple_of(task_first[t], 32), chunk), :HEAD]
        out[...] = lax.dot_general(
            q_all[task_span[t]], k, (((1,), (1,)), ((), ())), preferred_element_type=jnp.float32
        )

    def weigh(t, s_ref, p_ref, f_ref):
        i, k0 = task_span[t], task_first[t]
        low = low_all[i] - k0
        high = jnp.minimum(high_all[i], task_upper[t] - 1) - k0
        lane = lax.broadcasted_iota(jnp.int32, (SPAN, HEAD), 1)
        seen = [(lane >= low - g * HEAD) & (lane <= high - g * HEAD) for g in range(lanes)]
        for h in range(GROUP):
            at = slice(h * SPAN, (h + 1) * SPAN)
            s = [
                jnp.where(seen[g], s_ref[at, g * HEAD : (g + 1) * HEAD], 2 * LOW) for g in range(lanes)
            ]
            top = s[0]
            for g in range(1, lanes):
                top = jnp.maximum(top, s[g])
            best = best_all[i, at, :]
            new_best = jnp.maximum(best, jnp.max(top, axis=1, keepdims=True))
            best_all[i, at, :] = new_best
            f_ref[at, :] = jnp.exp2((best - new_best) * FACTOR)
            for g in range(lanes):
                p_ref[at, g * HEAD : (g + 1) * HEAD] = jnp.exp2((s[g] - new_best) * FACTOR).astype(
                    jnp.bfloat16
                )

    def accumulate(t, p_ref, f_ref):
        i, k0 = task_span[t], pl.multiple_of(task_first[t], 32)
        v = jnp.concatenate([kv[pl.ds(k0, chunk), HEAD:], ones], axis=1)
        part = jnp.dot(p_ref[...], v, preferred_element_type=jnp.float32)
        fade = f_ref[...]
        for half in range(2):
            cols = slice(half * HEAD, (half + 1) * HEAD)
            acc_all[i, :, cols] = acc_all[i, :, cols] * fade + part[:, cols]

    score(1, s0)

    def pair(j, _):
        t = 2 * j + 1
        accumulate(t - 1, p1, f1)
        score(t + 1, s1)
        weigh(t, s0, p0, f0)
        accumulate(t, p0, f0)
        score(t + 2, s0)
        weigh(t + 1, s1, p1, f1)
        return 0

    pairs = total // 2
    lax.fori_loop(0, pairs, pair, 0)
    accumulate(2 * pairs, p1, f1)

    if first_phase:
        weight_copy.wait()
    if last_phase:
        for turn in range(2):
            half = 1 - core if turn == 0 else core
            for s in range(RING):
                i = 2 * s + half
                for h in range(GROUP):
                    at = slice(h * SPAN, (h + 1) * SPAN)
                    outs[4 * turn + s][:, h * HEAD : (h + 1) * HEAD] = (
                        acc_all[i, at, :HEAD] / acc_all[i, at, HEAD:]
                    ).astype(jnp.bfloat16)


def run_phase(phase, scalars, pieces, others, weight=None):
    smem = pl.BlockSpec(memory_space=pltpu.SMEM)
    vmem = pl.BlockSpec(memory_space=pltpu.VMEM)
    chunk = CHUNKS[phase]
    keys = sum(piece.shape[0] for piece in pieces)
    state = [((8, ROWS, HEAD), jnp.float32), ((8, ROWS, 2 * HEAD), jnp.float32)]
    far = [] if weight is None else [weight]
    held = [(w.shape, w.dtype) for w in far]
    if phase == 0:
        outs = [((8, ROWS, HEAD), jnp.bfloat16)] + state + held
        aliases = {}
    else:
        outs = state + held
        first = 4 + len(pieces) + 1
        aliases = {first: 0, first + 1: 1}
    if phase == 3:
        outs = outs + [((SPAN, GROUP * HEAD), jnp.bfloat16)] * 8
    scratch = [
        pltpu.VMEM((keys, 2 * HEAD), jnp.bfloat16),
        pltpu.VMEM((8, SPAN, HEAD), jnp.int32),
        pltpu.VMEM((8, SPAN, HEAD), jnp.int32),
        pltpu.VMEM((ROWS, chunk), jnp.float32),
        pltpu.VMEM((ROWS, chunk), jnp.float32),
        pltpu.VMEM((ROWS, chunk), jnp.bfloat16),
        pltpu.VMEM((ROWS, chunk), jnp.bfloat16),
        pltpu.VMEM((ROWS, HEAD), jnp.float32),
        pltpu.VMEM((ROWS, HEAD), jnp.float32),
        pltpu.SMEM((MAX_TASKS,), jnp.int32),
        pltpu.SMEM((MAX_TASKS,), jnp.int32),
        pltpu.SMEM((MAX_TASKS,), jnp.int32),
    ] + [pltpu.SemaphoreType.DMA] * len(far)
    share = len(pieces) / 16
    return pl.pallas_call(
        lambda *refs: phase_kernel(phase, *refs),
        out_shape=[jax.ShapeDtypeStruct(*o) for o in outs],
        in_specs=[smem] * 4
        + [vmem] * (len(pieces) + len(others))
        + [pl.BlockSpec(memory_space=pltpu.HBM)] * len(far),
        out_specs=[vmem] * len(outs),
        scratch_shapes=scratch,
        input_output_aliases=aliases,
        compiler_params=pltpu.CompilerParams(vmem_limit_bytes=16 * 1024 * 1024),
        cost_estimate=pl.CostEstimate(
            flops=int(8e9 * share), bytes_accessed=int(1e7 * share), transcendentals=int(1e7 * share)
        ),
    )(*scalars, *pieces, *others, *far)


def project_kernel(coords, o0, o1, o2, o3, w, out):
    y = coords[2]
    block = 512
    for n in range(w.shape[1] // block):
        cols = slice(n * block, (n + 1) * block)
        acc = None
        for s, ref in enumerate((o0, o1, o2, o3)):
            row = pl.multiple_of(((y + s) % RING) * 512, 512)
            part = jnp.dot(ref[...], w[pl.ds(row, 512), cols], preferred_element_type=jnp.float32)
            acc = part if acc is None else acc + part
        out[:, cols] = acc.astype(out.dtype)


def project(coords, o_parts, weight, dtype):
    smem = pl.BlockSpec(memory_space=pltpu.SMEM)
    vmem = pl.BlockSpec(memory_space=pltpu.VMEM)
    width = weight.shape[1]
    return pl.pallas_call(
        project_kernel,
        out_shape=jax.ShapeDtypeStruct((SPAN, width), dtype),
        in_specs=[smem] + [vmem] * 5,
        out_specs=vmem,
        compiler_params=pltpu.CompilerParams(vmem_limit_bytes=16 * 1024 * 1024),
        cost_estimate=pl.CostEstimate(
            flops=2 * SPAN * 2048 * width, bytes_accessed=2048 * width * 2, transcendentals=0
        ),
        name="project",
    )(coords, *o_parts, weight)


def layer(queries, keys, values, span_table, doc_ids, out_weight):
    rows = queries.shape[0]
    spans = span_table.shape[0]
    x, z, y, core = (lax.axis_index(a) for a in ("x", "z", "y", "hd"))
    coords = jnp.stack([x, z, y, core]).astype(jnp.int32)
    kv = jnp.concatenate([keys.reshape(rows, RING, HEAD), values.reshape(rows, RING, HEAD)], axis=2)
    kv = kv.transpose(1, 0, 2)
    part = [lax.dynamic_index_in_dim(kv, (y + s) % RING, 0, keepdims=False) for s in range(RING)]
    part = [part[0]] + [shift(part[s], "y", s) for s in range(1, RING)]
    low, high = jnp.concatenate(part[:2], 0), jnp.concatenate(part[2:], 0)

    q_part = [
        lax.dynamic_slice_in_dim(queries, ((y + s) % RING) * 512, 512, 1) for s in range(RING)
    ]
    q_part = [q_part[0]] + [shift(q_part[s], "y", s) for s in range(1, RING)]

    def gathered(block, near_axis, far_axis):
        near = [block] + [shift(block, near_axis, s) for s in range(1, RING)]
        first, second = jnp.concatenate(near[:2], 0), jnp.concatenate(near[2:], 0)
        ahead_first = shift(first, far_axis, 1)
        behind_second = shift(second, far_axis, -1)
        ahead_second = shift(second, far_axis, 1)
        behind_first = shift(first, far_axis, -1)
        far_first = shift(ahead_first, far_axis, 1)
        far_second = shift(behind_second, far_axis, -1)
        return [first, second], [ahead_first, behind_second], [ahead_second, behind_first], [far_first, far_second]

    pieces = [a + b for a, b in zip(gathered(low, "z", "x"), gathered(high, "x", "z"))]

    docs = jnp.arange(DOCS, dtype=jnp.int32)
    starts = jnp.sum((doc_ids[None, :] < docs[:, None]).astype(jnp.int32), axis=1)
    slot = jnp.arange(spans, dtype=jnp.int32)
    cp = slot // 2
    dx, dz, dy = (x - cp // 16) % RING, (z - (cp // 4) % 4) % RING, (y - cp % 4) % RING
    far, near = jnp.where(dy < 2, dx, dz), jnp.where(dy < 2, dz, dx)
    early = (far == 1) == (near < 2)
    phase_of = jnp.where(far == 0, 0, jnp.where(far == 2, 3, jnp.where(early, 1, 2)))
    before = span_table[None, :] < jnp.arange(spans + 8, dtype=jnp.int32)[:, None]
    ranks = [jnp.sum((before & (phase_of == p)[None, :]).astype(jnp.int32), axis=1) for p in range(4)]

    scalars = [coords, span_table, starts]
    q_all, best, acc, weight = run_phase(0, scalars + [ranks[0]], pieces[0], q_part, out_weight)
    best, acc = run_phase(1, scalars + [ranks[1]], pieces[1], [q_all, best, acc])
    best, acc = run_phase(2, scalars + [ranks[2]], pieces[2], [q_all, best, acc])
    o_part = run_phase(3, scalars + [ranks[3]], pieces[3], [q_all, best, acc])[2:]

    def returned(part):
        return [part[0]] + [shift(part[s], "y", -s) for s in range(1, RING)]

    theirs, ours = returned(o_part[:4]), returned(o_part[4:])
    sent = lax.ppermute(project(coords, theirs, weight, jnp.bfloat16), "hd", [(0, 1), (1, 0)])
    kept = project(coords, ours, weight, jnp.float32)
    return (kept + sent.astype(jnp.float32)).astype(jnp.bfloat16)


def solution(mesh):
    inner = Mesh(mesh.devices.reshape(RING, RING, RING, 2), ("x", "z", "y", "hd"))
    cp = ("x", "z", "y")
    return jax.shard_map(
        layer,
        mesh=inner,
        in_specs=(P(cp, "hd"), P(cp, "hd"), P(cp, "hd"), P(), P(), P("hd", None)),
        out_specs=P(cp + ("hd",), None),
        check_vma=False,
    )
```

```python
import jax
import jax.numpy as jnp
from jax import lax
from jax.experimental import pallas as pl
from jax.experimental.pallas import tpu as pltpu
from jax.sharding import Mesh, PartitionSpec as P

HEAD = 128
SPAN = 96
RING = 4
GROUP = 4
ROWS = GROUP * SPAN
DOCS = 8
LOW = -1e30
LOG2E = 1.4426950408889634
FACTOR = HEAD ** -0.5 * LOG2E
MAX_TASKS = 160

PHASES = (((0, 0), (0, 1)), ((1, 0), (1, 1), (3, 0), (3, 1)), ((2, 0), (2, 1)))
CHUNKS = (256, 512, 256)


def shift(value, axis, by):
    return lax.ppermute(value, axis, [(i, (i + by) % RING) for i in range(RING)])


def phase_kernel(phase, *refs):
    chunk = CHUNKS[phase]
    first_phase, last_phase = phase == 0, phase == 2
    order = PHASES[phase]
    refs = list(refs)

    def take(n):
        out = refs[:n]
        del refs[:n]
        return out

    coords, table, starts, rank = take(4)
    pieces = take(2 * len(order))
    if first_phase:
        q_parts = take(4)
    else:
        (q_all,) = take(1)
        take(2)
    if first_phase:
        (weight,) = take(1)
        (q_all,) = take(1)
    best_all, acc_all = take(2)
    if last_phase:
        outs = take(8)
    if first_phase:
        (weight_held,) = take(1)
        weight_copy = pltpu.make_async_copy(weight, weight_held, refs.pop())
        weight_copy.start()
    kv, low_all, high_all, s0, s1, p0, p1, f0, f1, task_span, task_first, task_upper = refs
    x, z, y, core = coords[0], coords[1], coords[2], coords[3]

    def slot_of(dx, dz, dy, half):
        cp = ((x + RING - dx) % RING) * 16 + ((z + RING - dz) % RING) * 4 + (y + RING - dy) % RING
        return 2 * cp + half

    for family in range(2):
        for index, (far, upper_block) in enumerate(order):
            ref = pieces[family * len(order) + index]
            for i in range(8):
                near = 2 * upper_block + i // 4
                dy = 2 * family + (i // 2) % 2
                dx, dz = (far, near) if family == 0 else (near, far)
                row = rank[table[slot_of(dx, dz, dy, i % 2)]] * SPAN
                kv[pl.ds(pl.multiple_of(row, SPAN), SPAN), :] = ref[i * SPAN : (i + 1) * SPAN, :]

    if first_phase:
        for s, ref in enumerate(q_parts):
            for half in range(2):
                for h in range(GROUP):
                    q_all[2 * s + half, h * SPAN : (h + 1) * SPAN, :] = ref[
                        half * SPAN : (half + 1) * SPAN, h * HEAD : (h + 1) * HEAD
                    ]
        best_all[...] = jnp.full(best_all.shape, LOW, jnp.float32)
        acc_all[...] = jnp.zeros(acc_all.shape, jnp.float32)

    doc_low = []
    for d in range(DOCS):
        span = starts[d] // SPAN
        doc_low.append(rank[span] * SPAN + (rank[span + 1] - rank[span]) * (starts[d] - span * SPAN))

    def plan(i, total):
        span = table[slot_of(0, 0, i // 2, i % 2)]
        row = lax.broadcasted_iota(jnp.int32, (SPAN, HEAD), 0)
        low = jnp.full((SPAN, HEAD), doc_low[0], jnp.int32)
        low_min = doc_low[0]
        for d in range(1, DOCS):
            low = jnp.where(row >= starts[d] - span * SPAN, doc_low[d], low)
            low_min = jnp.where(starts[d] <= span * SPAN, doc_low[d], low_min)
        low_all[i] = low
        base, top = rank[span] * SPAN, rank[span + 1] * SPAN
        high_all[i] = jnp.where(top > base, base + row, base - 1)

        def add(e, n):
            task_span[n] = i
            task_upper[n] = top - e * chunk
            task_first[n] = jnp.maximum(top - (e + 1) * chunk, 0)
            return n + 1

        return lax.fori_loop(0, (top - low_min + chunk - 1) // chunk, add, total)

    total = lax.fori_loop(0, 8, plan, 1)
    task_span[0] = 0
    task_first[0] = 0
    for extra in range(3):
        task_span[total + extra] = 0
        task_first[total + extra] = 0
        task_upper[total + extra] = 0

    p1[...] = jnp.zeros(p1.shape, jnp.bfloat16)
    f1[...] = jnp.ones(f1.shape, jnp.float32)
    ones = jnp.ones((chunk, HEAD), jnp.bfloat16)
    lanes = chunk // HEAD

    def score(t, out):
        k = kv[pl.ds(pl.multiple_of(task_first[t], 32), chunk), :HEAD]
        out[...] = lax.dot_general(
            q_all[task_span[t]], k, (((1,), (1,)), ((), ())), preferred_element_type=jnp.float32
        )

    def weigh(t, s_ref, p_ref, f_ref):
        i, k0 = task_span[t], task_first[t]
        low = low_all[i] - k0
        high = jnp.minimum(high_all[i], task_upper[t] - 1) - k0
        lane = lax.broadcasted_iota(jnp.int32, (SPAN, HEAD), 1)
        seen = [(lane >= low - g * HEAD) & (lane <= high - g * HEAD) for g in range(lanes)]
        for h in range(GROUP):
            at = slice(h * SPAN, (h + 1) * SPAN)
            s = [
                jnp.where(seen[g], s_ref[at, g * HEAD : (g + 1) * HEAD], 2 * LOW) for g in range(lanes)
            ]
            top = s[0]
            for g in range(1, lanes):
                top = jnp.maximum(top, s[g])
            best = best_all[i, at, :]
            new_best = jnp.maximum(best, jnp.max(top, axis=1, keepdims=True))
            best_all[i, at, :] = new_best
            f_ref[at, :] = jnp.exp2((best - new_best) * FACTOR)
            for g in range(lanes):
                p_ref[at, g * HEAD : (g + 1) * HEAD] = jnp.exp2((s[g] - new_best) * FACTOR).astype(
                    jnp.bfloat16
                )

    def accumulate(t, p_ref, f_ref):
        i, k0 = task_span[t], pl.multiple_of(task_first[t], 32)
        v = jnp.concatenate([kv[pl.ds(k0, chunk), HEAD:], ones], axis=1)
        part = jnp.dot(p_ref[...], v, preferred_element_type=jnp.float32)
        fade = f_ref[...]
        for half in range(2):
            cols = slice(half * HEAD, (half + 1) * HEAD)
            acc_all[i, :, cols] = acc_all[i, :, cols] * fade + part[:, cols]

    score(1, s0)

    def pair(j, _):
        t = 2 * j + 1
        accumulate(t - 1, p1, f1)
        score(t + 1, s1)
        weigh(t, s0, p0, f0)
        accumulate(t, p0, f0)
        score(t + 2, s0)
        weigh(t + 1, s1, p1, f1)
        return 0

    pairs = total // 2
    lax.fori_loop(0, pairs, pair, 0)
    accumulate(2 * pairs, p1, f1)

    if first_phase:
        weight_copy.wait()
    if last_phase:
        for turn in range(2):
            half = 1 - core if turn == 0 else core
            for s in range(RING):
                i = 2 * s + half
                for h in range(GROUP):
                    at = slice(h * SPAN, (h + 1) * SPAN)
                    outs[4 * turn + s][:, h * HEAD : (h + 1) * HEAD] = (
                        acc_all[i, at, :HEAD] / acc_all[i, at, HEAD:]
                    ).astype(jnp.bfloat16)


def run_phase(phase, scalars, pieces, others, weight=None):
    smem = pl.BlockSpec(memory_space=pltpu.SMEM)
    vmem = pl.BlockSpec(memory_space=pltpu.VMEM)
    chunk = CHUNKS[phase]
    keys = sum(piece.shape[0] for piece in pieces)
    state = [((8, ROWS, HEAD), jnp.float32), ((8, ROWS, 2 * HEAD), jnp.float32)]
    far = [] if weight is None else [weight]
    held = [(w.shape, w.dtype) for w in far]
    if phase == 0:
        outs = [((8, ROWS, HEAD), jnp.bfloat16)] + state + held
        aliases = {}
    else:
        outs = state + held
        first = 4 + len(pieces) + 1
        aliases = {first: 0, first + 1: 1}
    if phase == 2:
        outs = outs + [((SPAN, GROUP * HEAD), jnp.bfloat16)] * 8
    scratch = [
        pltpu.VMEM((keys, 2 * HEAD), jnp.bfloat16),
        pltpu.VMEM((8, SPAN, HEAD), jnp.int32),
        pltpu.VMEM((8, SPAN, HEAD), jnp.int32),
        pltpu.VMEM((ROWS, chunk), jnp.float32),
        pltpu.VMEM((ROWS, chunk), jnp.float32),
        pltpu.VMEM((ROWS, chunk), jnp.bfloat16),
        pltpu.VMEM((ROWS, chunk), jnp.bfloat16),
        pltpu.VMEM((ROWS, HEAD), jnp.float32),
        pltpu.VMEM((ROWS, HEAD), jnp.float32),
        pltpu.SMEM((MAX_TASKS,), jnp.int32),
        pltpu.SMEM((MAX_TASKS,), jnp.int32),
        pltpu.SMEM((MAX_TASKS,), jnp.int32),
    ] + [pltpu.SemaphoreType.DMA] * len(far)
    share = len(pieces) / 16
    return pl.pallas_call(
        lambda *refs: phase_kernel(phase, *refs),
        out_shape=[jax.ShapeDtypeStruct(*o) for o in outs],
        in_specs=[smem] * 4
        + [vmem] * (len(pieces) + len(others))
        + [pl.BlockSpec(memory_space=pltpu.HBM)] * len(far),
        out_specs=[vmem] * len(outs),
        scratch_shapes=scratch,
        input_output_aliases=aliases,
        compiler_params=pltpu.CompilerParams(vmem_limit_bytes=16 * 1024 * 1024),
        cost_estimate=pl.CostEstimate(
            flops=int(8e9 * share), bytes_accessed=int(1e7 * share), transcendentals=int(1e7 * share)
        ),
    )(*scalars, *pieces, *others, *far)


def project_kernel(coords, o0, o1, o2, o3, w, out):
    y = coords[2]
    block = 512
    for n in range(w.shape[1] // block):
        cols = slice(n * block, (n + 1) * block)
        acc = None
        for s, ref in enumerate((o0, o1, o2, o3)):
            row = pl.multiple_of(((y + s) % RING) * 512, 512)
            part = jnp.dot(ref[...], w[pl.ds(row, 512), cols], preferred_element_type=jnp.float32)
            acc = part if acc is None else acc + part
        out[:, cols] = acc.astype(out.dtype)


def project(coords, o_parts, weight, dtype):
    smem = pl.BlockSpec(memory_space=pltpu.SMEM)
    vmem = pl.BlockSpec(memory_space=pltpu.VMEM)
    width = weight.shape[1]
    return pl.pallas_call(
        project_kernel,
        out_shape=jax.ShapeDtypeStruct((SPAN, width), dtype),
        in_specs=[smem] + [vmem] * 5,
        out_specs=vmem,
        compiler_params=pltpu.CompilerParams(vmem_limit_bytes=16 * 1024 * 1024),
        cost_estimate=pl.CostEstimate(
            flops=2 * SPAN * 2048 * width, bytes_accessed=2048 * width * 2, transcendentals=0
        ),
        name="project",
    )(coords, *o_parts, weight)


def layer(queries, keys, values, span_table, doc_ids, out_weight):
    rows = queries.shape[0]
    spans = span_table.shape[0]
    x, z, y, core = (lax.axis_index(a) for a in ("x", "z", "y", "hd"))
    coords = jnp.stack([x, z, y, core]).astype(jnp.int32)
    kv = jnp.concatenate([keys.reshape(rows, RING, HEAD), values.reshape(rows, RING, HEAD)], axis=2)
    kv = kv.transpose(1, 0, 2)
    part = [lax.dynamic_index_in_dim(kv, (y + s) % RING, 0, keepdims=False) for s in range(RING)]
    part = [part[0]] + [shift(part[s], "y", s) for s in range(1, RING)]
    low, high = jnp.concatenate(part[:2], 0), jnp.concatenate(part[2:], 0)

    q_part = [
        lax.dynamic_slice_in_dim(queries, ((y + s) % RING) * 512, 512, 1) for s in range(RING)
    ]
    q_part = [q_part[0]] + [shift(q_part[s], "y", s) for s in range(1, RING)]

    def gathered(block, near_axis, far_axis):
        near = [block] + [shift(block, near_axis, s) for s in range(1, RING)]
        first, second = jnp.concatenate(near[:2], 0), jnp.concatenate(near[2:], 0)
        ahead_first = shift(first, far_axis, 1)
        behind_second = shift(second, far_axis, -1)
        ahead_second = shift(second, far_axis, 1)
        behind_first = shift(first, far_axis, -1)
        far_first = shift(ahead_first, far_axis, 1)
        far_second = shift(behind_second, far_axis, -1)
        return [first, second], [ahead_first, ahead_second, behind_first, behind_second], [far_first, far_second]

    pieces = [a + b for a, b in zip(gathered(low, "z", "x"), gathered(high, "x", "z"))]

    docs = jnp.arange(DOCS, dtype=jnp.int32)
    starts = jnp.sum((doc_ids[None, :] < docs[:, None]).astype(jnp.int32), axis=1)
    slot = jnp.arange(spans, dtype=jnp.int32)
    cp = slot // 2
    dx, dz, dy = (x - cp // 16) % RING, (z - (cp // 4) % 4) % RING, (y - cp % 4) % RING
    far = jnp.where(dy < 2, dx, dz)
    phase_of = jnp.where(far == 0, 0, jnp.where(far == 2, 2, 1))
    before = span_table[None, :] < jnp.arange(spans + 8, dtype=jnp.int32)[:, None]
    ranks = [jnp.sum((before & (phase_of == p)[None, :]).astype(jnp.int32), axis=1) for p in range(3)]

    scalars = [coords, span_table, starts]
    q_all, best, acc, weight = run_phase(0, scalars + [ranks[0]], pieces[0], q_part, out_weight)
    best, acc = run_phase(1, scalars + [ranks[1]], pieces[1], [q_all, best, acc])
    o_part = run_phase(2, scalars + [ranks[2]], pieces[2], [q_all, best, acc])[2:]

    def returned(part):
        return [part[0]] + [shift(part[s], "y", -s) for s in range(1, RING)]

    theirs, ours = returned(o_part[:4]), returned(o_part[4:])
    sent = lax.ppermute(project(coords, theirs, weight, jnp.bfloat16), "hd", [(0, 1), (1, 0)])
    kept = project(coords, ours, weight, jnp.float32)
    return (kept + sent.astype(jnp.float32)).astype(jnp.bfloat16)


def solution(mesh):
    inner = Mesh(mesh.devices.reshape(RING, RING, RING, 2), ("x", "z", "y", "hd"))
    cp = ("x", "z", "y")
    return jax.shard_map(
        layer,
        mesh=inner,
        in_specs=(P(cp, "hd"), P(cp, "hd"), P(cp, "hd"), P(), P(), P("hd", None)),
        out_specs=P(cp + ("hd",), None),
        check_vma=False,
    )
```

```python
import jax
import jax.numpy as jnp
from jax import lax
from jax.experimental import pallas as pl
from jax.experimental.pallas import tpu as pltpu
from jax.sharding import Mesh, PartitionSpec as P

HEAD = 128
SPAN = 96
RING = 4
GROUP = 4
ROWS = GROUP * SPAN
DOCS = 8
LOW = -1e30
LOG2E = 1.4426950408889634
FACTOR = HEAD ** -0.5 * LOG2E
MAX_TASKS = 160
TILE = 16

PHASES = (((0, 0), (0, 1)), ((1, 0), (1, 1), (3, 0), (3, 1)), ((2, 0), (2, 1)))
CHUNKS = (256, 512, 256)


def shift(value, axis, by):
    return lax.ppermute(value, axis, [(i, (i + by) % RING) for i in range(RING)])


def phase_kernel(phase, *refs):
    chunk = CHUNKS[phase]
    first_phase, last_phase = phase == 0, phase == 2
    order = PHASES[phase]
    refs = list(refs)

    def take(n):
        out = refs[:n]
        del refs[:n]
        return out

    coords, table, starts, rank = take(4)
    pieces = take(2 * len(order))
    if first_phase:
        q_parts = take(4)
    else:
        (q_all,) = take(1)
        take(2)
    if first_phase:
        (weight,) = take(1)
        (q_all,) = take(1)
    best_all, acc_all = take(2)
    if last_phase:
        outs = take(7)
    if first_phase:
        (weight_held,) = take(1)
        weight_copy = pltpu.make_async_copy(weight, weight_held, refs.pop())
        weight_copy.start()
    kv, low_all, high_all, s0, s1, p0, p1, f0, f1, task_span, task_first, task_upper = refs
    x, z, y, core = coords[0], coords[1], coords[2], coords[3]

    def slot_of(dx, dz, dy, half):
        cp = ((x + RING - dx) % RING) * 16 + ((z + RING - dz) % RING) * 4 + (y + RING - dy) % RING
        return 2 * cp + half

    for family in range(2):
        for index, (far, upper_block) in enumerate(order):
            ref = pieces[family * len(order) + index]
            for i in range(8):
                near = 2 * upper_block + i // 4
                dy = 2 * family + (i // 2) % 2
                dx, dz = (far, near) if family == 0 else (near, far)
                row = rank[table[slot_of(dx, dz, dy, i % 2)]] * SPAN
                kv[pl.ds(pl.multiple_of(row, SPAN), SPAN), :] = ref[i * SPAN : (i + 1) * SPAN, :]

    if first_phase:
        for s, ref in enumerate(q_parts):
            for half in range(2):
                for h in range(GROUP):
                    scaled = ref[half * SPAN : (half + 1) * SPAN, h * HEAD : (h + 1) * HEAD]
                    scaled = scaled.astype(jnp.float32) * FACTOR
                    main = scaled.astype(jnp.bfloat16)
                    rest = (scaled - main.astype(jnp.float32)).astype(jnp.bfloat16)
                    q_all[2 * s + half, h * SPAN : (h + 1) * SPAN, :HEAD] = main
                    q_all[2 * s + half, h * SPAN : (h + 1) * SPAN, HEAD:] = rest
        best_all[...] = jnp.full(best_all.shape, LOW, jnp.float32)
        acc_all[...] = jnp.zeros(acc_all.shape, jnp.float32)

    doc_low = []
    for d in range(DOCS):
        span = starts[d] // SPAN
        doc_low.append(rank[span] * SPAN + (rank[span + 1] - rank[span]) * (starts[d] - span * SPAN))

    def plan(i, total):
        span = table[slot_of(0, 0, i // 2, i % 2)]
        row = lax.broadcasted_iota(jnp.int32, (SPAN, HEAD), 0)
        low = jnp.full((SPAN, HEAD), doc_low[0], jnp.int32)
        low_min = doc_low[0]
        for d in range(1, DOCS):
            low = jnp.where(row >= starts[d] - span * SPAN, doc_low[d], low)
            low_min = jnp.where(starts[d] <= span * SPAN, doc_low[d], low_min)
        low_all[i] = low
        base, top = rank[span] * SPAN, rank[span + 1] * SPAN
        high_all[i] = jnp.where(top > base, base + row, base - 1)

        def add(e, n):
            task_span[n] = i
            task_upper[n] = top - e * chunk
            task_first[n] = jnp.maximum(top - (e + 1) * chunk, 0)
            return n + 1

        return lax.fori_loop(0, (top - low_min + chunk - 1) // chunk, add, total)

    total = lax.fori_loop(0, 8, plan, 1)
    task_span[0] = 0
    task_first[0] = 0
    for extra in range(3):
        task_span[total + extra] = 0
        task_first[total + extra] = 0
        task_upper[total + extra] = 0

    p1[...] = jnp.zeros(p1.shape, jnp.bfloat16)
    f1[...] = jnp.ones(f1.shape, jnp.float32)
    ones = jnp.ones((chunk, HEAD), jnp.bfloat16)
    lanes = chunk // HEAD

    def score(t, out):
        k = kv[pl.ds(pl.multiple_of(task_first[t], 32), chunk), :HEAD]
        out[...] = lax.dot_general(
            q_all[task_span[t]], jnp.concatenate([k, k], axis=1), (((1,), (1,)), ((), ())), preferred_element_type=jnp.float32
        )

    def weigh(t, s_ref, p_ref, f_ref):
        i, k0 = task_span[t], task_first[t]
        last = task_upper[t] - 1
        lane = lax.broadcasted_iota(jnp.int32, (TILE, HEAD), 1)
        for r in range(0, SPAN, TILE):
            low = low_all[i, r : r + TILE, :] - k0
            high = jnp.minimum(high_all[i, r : r + TILE, :], last) - k0
            seen = [(lane + g * HEAD >= low) & (lane + g * HEAD <= high) for g in range(lanes)]
            for h in range(GROUP):
                at = slice(h * SPAN + r, h * SPAN + r + TILE)
                s = [
                    jnp.where(seen[g], s_ref[at, g * HEAD : (g + 1) * HEAD], 2 * LOW)
                    for g in range(lanes)
                ]
                top = s[0]
                for g in range(1, lanes):
                    top = jnp.maximum(top, s[g])
                best = best_all[i, at, :]
                new_best = jnp.maximum(best, jnp.max(top, axis=1, keepdims=True))
                best_all[i, at, :] = new_best
                f_ref[at, :] = jnp.exp2(best - new_best)
                p_ref[at, :] = jnp.concatenate([jnp.exp2(x - new_best) for x in s], axis=1).astype(
                    jnp.bfloat16
                )

    def accumulate(t, p_ref, f_ref):
        i, k0 = task_span[t], pl.multiple_of(task_first[t], 32)
        v = jnp.concatenate([kv[pl.ds(k0, chunk), HEAD:], ones], axis=1)
        part = jnp.dot(p_ref[...], v, preferred_element_type=jnp.float32)
        fade = f_ref[...]
        for half in range(2):
            cols = slice(half * HEAD, (half + 1) * HEAD)
            acc_all[i, :, cols] = acc_all[i, :, cols] * fade + part[:, cols]

    score(1, s0)

    def pair(j, _):
        t = 2 * j + 1
        accumulate(t - 1, p1, f1)
        score(t + 1, s1)
        weigh(t, s0, p0, f0)
        accumulate(t, p0, f0)
        score(t + 2, s0)
        weigh(t + 1, s1, p1, f1)
        return 0

    pairs = total // 2
    lax.fori_loop(0, pairs, pair, 0)
    accumulate(2 * pairs, p1, f1)

    if first_phase:
        weight_copy.wait()
    if last_phase:
        for turn in range(2):
            half = 1 - core if turn == 0 else core
            for s in range(RING):
                i = 2 * s + half
                out = outs[6] if s == 2 else outs[3 * turn + min(s, 2)]
                first = turn * SPAN if s == 2 else 0
                for h in range(GROUP):
                    at = slice(h * SPAN, (h + 1) * SPAN)
                    out[first : first + SPAN, h * HEAD : (h + 1) * HEAD] = (
                        acc_all[i, at, :HEAD] / acc_all[i, at, HEAD:]
                    ).astype(jnp.bfloat16)


def run_phase(phase, scalars, pieces, others, weight=None):
    smem = pl.BlockSpec(memory_space=pltpu.SMEM)
    vmem = pl.BlockSpec(memory_space=pltpu.VMEM)
    chunk = CHUNKS[phase]
    keys = sum(piece.shape[0] for piece in pieces)
    state = [((8, ROWS, HEAD), jnp.float32), ((8, ROWS, 2 * HEAD), jnp.float32)]
    far = [] if weight is None else [weight]
    held = [(w.shape, w.dtype) for w in far]
    if phase == 0:
        outs = [((8, ROWS, 2 * HEAD), jnp.bfloat16)] + state + held
        aliases = {}
    else:
        outs = state + held
        first = 4 + len(pieces) + 1
        aliases = {first: 0, first + 1: 1}
    if phase == 2:
        part = ((SPAN, GROUP * HEAD), jnp.bfloat16)
        outs = outs + [part] * 6 + [((2 * SPAN, GROUP * HEAD), jnp.bfloat16)]
    scratch = [
        pltpu.VMEM((keys, 2 * HEAD), jnp.bfloat16),
        pltpu.VMEM((8, SPAN, HEAD), jnp.int32),
        pltpu.VMEM((8, SPAN, HEAD), jnp.int32),
        pltpu.VMEM((ROWS, chunk), jnp.float32),
        pltpu.VMEM((ROWS, chunk), jnp.float32),
        pltpu.VMEM((ROWS, chunk), jnp.bfloat16),
        pltpu.VMEM((ROWS, chunk), jnp.bfloat16),
        pltpu.VMEM((ROWS, HEAD), jnp.float32),
        pltpu.VMEM((ROWS, HEAD), jnp.float32),
        pltpu.SMEM((MAX_TASKS,), jnp.int32),
        pltpu.SMEM((MAX_TASKS,), jnp.int32),
        pltpu.SMEM((MAX_TASKS,), jnp.int32),
    ] + [pltpu.SemaphoreType.DMA] * len(far)
    share = len(pieces) / 16
    return pl.pallas_call(
        lambda *refs: phase_kernel(phase, *refs),
        out_shape=[jax.ShapeDtypeStruct(*o) for o in outs],
        in_specs=[smem] * 4
        + [vmem] * (len(pieces) + len(others))
        + [pl.BlockSpec(memory_space=pltpu.HBM)] * len(far),
        out_specs=[vmem] * len(outs),
        scratch_shapes=scratch,
        input_output_aliases=aliases,
        compiler_params=pltpu.CompilerParams(vmem_limit_bytes=16 * 1024 * 1024),
        cost_estimate=pl.CostEstimate(
            flops=int(8e9 * share), bytes_accessed=int(1e7 * share), transcendentals=int(1e7 * share)
        ),
    )(*scalars, *pieces, *others, *far)


def project_kernel(turn, coords, o0, o1, o2, o3, w, out):
    y = coords[2]
    block = 512
    for n in range(w.shape[1] // block):
        cols = slice(n * block, (n + 1) * block)
        acc = None
        for s, ref in enumerate((o0, o1, o2, o3)):
            row = pl.multiple_of(((y + s) % RING) * 512, 512)
            rows = ref[turn * SPAN : (turn + 1) * SPAN, :] if s == 2 else ref[...]
            part = jnp.dot(rows, w[pl.ds(row, 512), cols], preferred_element_type=jnp.float32)
            acc = part if acc is None else acc + part
        out[:, cols] = acc.astype(out.dtype)


def project(turn, coords, o_parts, weight, dtype):
    smem = pl.BlockSpec(memory_space=pltpu.SMEM)
    vmem = pl.BlockSpec(memory_space=pltpu.VMEM)
    width = weight.shape[1]
    return pl.pallas_call(
        lambda *refs: project_kernel(turn, *refs),
        out_shape=jax.ShapeDtypeStruct((SPAN, width), dtype),
        in_specs=[smem] + [vmem] * 5,
        out_specs=vmem,
        compiler_params=pltpu.CompilerParams(vmem_limit_bytes=16 * 1024 * 1024),
        cost_estimate=pl.CostEstimate(
            flops=2 * SPAN * 2048 * width, bytes_accessed=2048 * width * 2, transcendentals=0
        ),
        name="project",
    )(coords, *o_parts, weight)


def layer(queries, keys, values, span_table, doc_ids, out_weight):
    rows = queries.shape[0]
    spans = span_table.shape[0]
    x, z, y, core = (lax.axis_index(a) for a in ("x", "z", "y", "hd"))
    coords = jnp.stack([x, z, y, core]).astype(jnp.int32)
    kv = jnp.concatenate([keys.reshape(rows, RING, HEAD), values.reshape(rows, RING, HEAD)], axis=2)
    kv = kv.transpose(1, 0, 2)
    part = [lax.dynamic_index_in_dim(kv, (y + s) % RING, 0, keepdims=False) for s in range(RING)]
    part = [part[0]] + [shift(part[s], "y", s) for s in range(1, RING)]
    low, high = jnp.concatenate(part[:2], 0), jnp.concatenate(part[2:], 0)

    q_part = [
        lax.dynamic_slice_in_dim(queries, ((y + s) % RING) * 512, 512, 1) for s in range(RING)
    ]
    q_part = [q_part[0]] + [shift(q_part[s], "y", s) for s in range(1, RING)]

    def gathered(block, near_axis, far_axis):
        near = [block] + [shift(block, near_axis, s) for s in range(1, RING)]
        first, second = jnp.concatenate(near[:2], 0), jnp.concatenate(near[2:], 0)
        ahead_first = shift(first, far_axis, 1)
        behind_second = shift(second, far_axis, -1)
        ahead_second = shift(second, far_axis, 1)
        behind_first = shift(first, far_axis, -1)
        far_first = shift(ahead_first, far_axis, 1)
        far_second = shift(behind_second, far_axis, -1)
        return [first, second], [ahead_first, ahead_second, behind_first, behind_second], [far_first, far_second]

    pieces = [a + b for a, b in zip(gathered(low, "z", "x"), gathered(high, "x", "z"))]

    docs = jnp.arange(DOCS, dtype=jnp.int32)
    starts = jnp.sum((doc_ids[None, :] < docs[:, None]).astype(jnp.int32), axis=1)
    slot = jnp.arange(spans, dtype=jnp.int32)
    cp = slot // 2
    dx, dz, dy = (x - cp // 16) % RING, (z - (cp // 4) % 4) % RING, (y - cp % 4) % RING
    far = jnp.where(dy < 2, dx, dz)
    phase_of = jnp.where(far == 0, 0, jnp.where(far == 2, 2, 1))
    before = span_table[None, :] < jnp.arange(spans + 8, dtype=jnp.int32)[:, None]
    ranks = [jnp.sum((before & (phase_of == p)[None, :]).astype(jnp.int32), axis=1) for p in range(3)]

    scalars = [coords, span_table, starts]
    q_all, best, acc, weight = run_phase(0, scalars + [ranks[0]], pieces[0], q_part, out_weight)
    best, acc = run_phase(1, scalars + [ranks[1]], pieces[1], [q_all, best, acc])
    o_part = run_phase(2, scalars + [ranks[2]], pieces[2], [q_all, best, acc])[2:]

    def returned(part):
        return [part[0], shift(part[1], "y", -1), both, shift(part[2], "y", 1)]

    both = shift(o_part[6], "y", -2)
    theirs, ours = returned(o_part[:3]), returned(o_part[3:6])
    sent = project(0, coords, theirs, weight, jnp.bfloat16)
    sent = lax.ppermute(sent, "hd", [(0, 1), (1, 0)])
    kept = project(1, coords, ours, weight, jnp.float32)
    return (kept + sent.astype(jnp.float32)).astype(jnp.bfloat16)


def solution(mesh):
    inner = Mesh(mesh.devices.reshape(RING, RING, RING, 2), ("x", "z", "y", "hd"))
    cp = ("x", "z", "y")
    return jax.shard_map(
        layer,
        mesh=inner,
        in_specs=(P(cp, "hd"), P(cp, "hd"), P(cp, "hd"), P(), P(), P("hd", None)),
        out_specs=P(cp + ("hd",), None),
        check_vma=False,
    )
```

```python
import jax
import jax.numpy as jnp
from jax import lax
from jax.experimental import pallas as pl
from jax.experimental.pallas import tpu as pltpu
from jax.sharding import Mesh, PartitionSpec as P

HEAD = 128
SPAN = 96
RING = 4
GROUP = 4
ROWS = GROUP * SPAN
DOCS = 8
LOW = -1e30
LOG2E = 1.4426950408889634
FACTOR = HEAD ** -0.5 * LOG2E
MAX_TASKS = 160
TILE = 16

PHASES = (((0, 0), (0, 1)), ((1, 0), (3, 1)), ((1, 1), (3, 0)), ((2, 0), (2, 1)))
CHUNKS = (256, 256, 256, 256)


def shift(value, axis, by):
    return lax.ppermute(value, axis, [(i, (i + by) % RING) for i in range(RING)])


def phase_kernel(phase, *refs):
    chunk = CHUNKS[phase]
    first_phase, last_phase = phase == 0, phase == 3
    order = PHASES[phase]
    refs = list(refs)

    def take(n):
        out = refs[:n]
        del refs[:n]
        return out

    coords, table, starts, rank = take(4)
    pieces = take(2 * len(order))
    if first_phase:
        q_parts = take(4)
    else:
        (q_all,) = take(1)
        take(2)
    if first_phase:
        (weight,) = take(1)
        (q_all,) = take(1)
    best_all, acc_all = take(2)
    if last_phase:
        outs = take(7)
    if first_phase:
        (weight_held,) = take(1)
        weight_copy = pltpu.make_async_copy(weight, weight_held, refs.pop())
        weight_copy.start()
    kv, low_all, high_all, s0, s1, p0, p1, f0, f1, task_span, task_first, task_upper = refs
    x, z, y, core = coords[0], coords[1], coords[2], coords[3]

    def slot_of(dx, dz, dy, half):
        cp = ((x + RING - dx) % RING) * 16 + ((z + RING - dz) % RING) * 4 + (y + RING - dy) % RING
        return 2 * cp + half

    for family in range(2):
        for index, (far, upper_block) in enumerate(order):
            ref = pieces[family * len(order) + index]
            for i in range(8):
                near = 2 * upper_block + i // 4
                dy = 2 * family + (i // 2) % 2
                dx, dz = (far, near) if family == 0 else (near, far)
                row = rank[table[slot_of(dx, dz, dy, i % 2)]] * SPAN
                kv[pl.ds(pl.multiple_of(row, SPAN), SPAN), :] = ref[i * SPAN : (i + 1) * SPAN, :]

    if first_phase:
        for s, ref in enumerate(q_parts):
            for half in range(2):
                for h in range(GROUP):
                    scaled = ref[half * SPAN : (half + 1) * SPAN, h * HEAD : (h + 1) * HEAD]
                    scaled = scaled.astype(jnp.float32) * FACTOR
                    main = scaled.astype(jnp.bfloat16)
                    rest = (scaled - main.astype(jnp.float32)).astype(jnp.bfloat16)
                    q_all[2 * s + half, h * SPAN : (h + 1) * SPAN, :HEAD] = main
                    q_all[2 * s + half, h * SPAN : (h + 1) * SPAN, HEAD:] = rest
        best_all[...] = jnp.full(best_all.shape, LOW, jnp.float32)
        acc_all[...] = jnp.zeros(acc_all.shape, jnp.float32)

    doc_low = []
    for d in range(DOCS):
        span = starts[d] // SPAN
        doc_low.append(rank[span] * SPAN + (rank[span + 1] - rank[span]) * (starts[d] - span * SPAN))

    def plan(i, total):
        span = table[slot_of(0, 0, i // 2, i % 2)]
        row = lax.broadcasted_iota(jnp.int32, (SPAN, HEAD), 0)
        low = jnp.full((SPAN, HEAD), doc_low[0], jnp.int32)
        low_min = doc_low[0]
        for d in range(1, DOCS):
            low = jnp.where(row >= starts[d] - span * SPAN, doc_low[d], low)
            low_min = jnp.where(starts[d] <= span * SPAN, doc_low[d], low_min)
        low_all[i] = low
        base, top = rank[span] * SPAN, rank[span + 1] * SPAN
        high_all[i] = jnp.where(top > base, base + row, base - 1)

        def add(e, n):
            task_span[n] = i
            task_upper[n] = top - e * chunk
            task_first[n] = jnp.maximum(top - (e + 1) * chunk, 0)
            return n + 1

        return lax.fori_loop(0, (top - low_min + chunk - 1) // chunk, add, total)

    total = lax.fori_loop(0, 8, plan, 1)
    task_span[0] = 0
    task_first[0] = 0
    for extra in range(3):
        task_span[total + extra] = 0
        task_first[total + extra] = 0
        task_upper[total + extra] = 0

    p1[...] = jnp.zeros(p1.shape, jnp.bfloat16)
    f1[...] = jnp.ones(f1.shape, jnp.float32)
    ones = jnp.ones((chunk, HEAD), jnp.bfloat16)
    lanes = chunk // HEAD

    def score(t, out):
        k = kv[pl.ds(pl.multiple_of(task_first[t], 32), chunk), :HEAD]
        out[...] = lax.dot_general(
            q_all[task_span[t]], jnp.concatenate([k, k], axis=1), (((1,), (1,)), ((), ())), preferred_element_type=jnp.float32
        )

    def weigh(t, s_ref, p_ref, f_ref):
        i, k0 = task_span[t], task_first[t]
        last = task_upper[t] - 1
        lane = lax.broadcasted_iota(jnp.int32, (TILE, HEAD), 1)
        for r in range(0, SPAN, TILE):
            low = low_all[i, r : r + TILE, :] - k0
            high = jnp.minimum(high_all[i, r : r + TILE, :], last) - k0
            seen = [(lane + g * HEAD >= low) & (lane + g * HEAD <= high) for g in range(lanes)]
            for h in range(GROUP):
                at = slice(h * SPAN + r, h * SPAN + r + TILE)
                s = [
                    jnp.where(seen[g], s_ref[at, g * HEAD : (g + 1) * HEAD], 2 * LOW)
                    for g in range(lanes)
                ]
                top = s[0]
                for g in range(1, lanes):
                    top = jnp.maximum(top, s[g])
                best = best_all[i, at, :]
                new_best = jnp.maximum(best, jnp.max(top, axis=1, keepdims=True))
                best_all[i, at, :] = new_best
                f_ref[at, :] = jnp.exp2(best - new_best)
                p_ref[at, :] = jnp.concatenate([jnp.exp2(x - new_best) for x in s], axis=1).astype(
                    jnp.bfloat16
                )

    def accumulate(t, p_ref, f_ref):
        i, k0 = task_span[t], pl.multiple_of(task_first[t], 32)
        v = jnp.concatenate([kv[pl.ds(k0, chunk), HEAD:], ones], axis=1)
        part = jnp.dot(p_ref[...], v, preferred_element_type=jnp.float32)
        fade = f_ref[...]
        for half in range(2):
            cols = slice(half * HEAD, (half + 1) * HEAD)
            acc_all[i, :, cols] = acc_all[i, :, cols] * fade + part[:, cols]

    score(1, s0)

    def pair(j, _):
        t = 2 * j + 1
        accumulate(t - 1, p1, f1)
        score(t + 1, s1)
        weigh(t, s0, p0, f0)
        accumulate(t, p0, f0)
        score(t + 2, s0)
        weigh(t + 1, s1, p1, f1)
        return 0

    pairs = total // 2
    lax.fori_loop(0, pairs, pair, 0)
    accumulate(2 * pairs, p1, f1)

    if first_phase:
        weight_copy.wait()
    if last_phase:
        for turn in range(2):
            half = 1 - core if turn == 0 else core
            for s in range(RING):
                i = 2 * s + half
                out = outs[6] if s == 2 else outs[3 * turn + min(s, 2)]
                first = turn * SPAN if s == 2 else 0
                for h in range(GROUP):
                    at = slice(h * SPAN, (h + 1) * SPAN)
                    out[first : first + SPAN, h * HEAD : (h + 1) * HEAD] = (
                        acc_all[i, at, :HEAD] / acc_all[i, at, HEAD:]
                    ).astype(jnp.bfloat16)


def run_phase(phase, scalars, pieces, others, weight=None):
    smem = pl.BlockSpec(memory_space=pltpu.SMEM)
    vmem = pl.BlockSpec(memory_space=pltpu.VMEM)
    chunk = CHUNKS[phase]
    keys = sum(piece.shape[0] for piece in pieces)
    state = [((8, ROWS, HEAD), jnp.float32), ((8, ROWS, 2 * HEAD), jnp.float32)]
    far = [] if weight is None else [weight]
    held = [(w.shape, w.dtype) for w in far]
    if phase == 0:
        outs = [((8, ROWS, 2 * HEAD), jnp.bfloat16)] + state + held
        aliases = {}
    else:
        outs = state + held
        first = 4 + len(pieces) + 1
        aliases = {first: 0, first + 1: 1}
    if phase == 3:
        part = ((SPAN, GROUP * HEAD), jnp.bfloat16)
        outs = outs + [part] * 6 + [((2 * SPAN, GROUP * HEAD), jnp.bfloat16)]
    scratch = [
        pltpu.VMEM((keys, 2 * HEAD), jnp.bfloat16),
        pltpu.VMEM((8, SPAN, HEAD), jnp.int32),
        pltpu.VMEM((8, SPAN, HEAD), jnp.int32),
        pltpu.VMEM((ROWS, chunk), jnp.float32),
        pltpu.VMEM((ROWS, chunk), jnp.float32),
        pltpu.VMEM((ROWS, chunk), jnp.bfloat16),
        pltpu.VMEM((ROWS, chunk), jnp.bfloat16),
        pltpu.VMEM((ROWS, HEAD), jnp.float32),
        pltpu.VMEM((ROWS, HEAD), jnp.float32),
        pltpu.SMEM((MAX_TASKS,), jnp.int32),
        pltpu.SMEM((MAX_TASKS,), jnp.int32),
        pltpu.SMEM((MAX_TASKS,), jnp.int32),
    ] + [pltpu.SemaphoreType.DMA] * len(far)
    share = len(pieces) / 16
    return pl.pallas_call(
        lambda *refs: phase_kernel(phase, *refs),
        out_shape=[jax.ShapeDtypeStruct(*o) for o in outs],
        in_specs=[smem] * 4
        + [vmem] * (len(pieces) + len(others))
        + [pl.BlockSpec(memory_space=pltpu.HBM)] * len(far),
        out_specs=[vmem] * len(outs),
        scratch_shapes=scratch,
        input_output_aliases=aliases,
        compiler_params=pltpu.CompilerParams(vmem_limit_bytes=16 * 1024 * 1024),
        cost_estimate=pl.CostEstimate(
            flops=int(8e9 * share), bytes_accessed=int(1e7 * share), transcendentals=int(1e7 * share)
        ),
    )(*scalars, *pieces, *others, *far)


def project_kernel(turn, coords, o0, o1, o2, o3, w, out):
    y = coords[2]
    block = 512
    for n in range(w.shape[1] // block):
        cols = slice(n * block, (n + 1) * block)
        acc = None
        for s, ref in enumerate((o0, o1, o2, o3)):
            row = pl.multiple_of(((y + s) % RING) * 512, 512)
            rows = ref[turn * SPAN : (turn + 1) * SPAN, :] if s == 2 else ref[...]
            part = jnp.dot(rows, w[pl.ds(row, 512), cols], preferred_element_type=jnp.float32)
            acc = part if acc is None else acc + part
        out[:, cols] = acc.astype(out.dtype)


def project(turn, coords, o_parts, weight, dtype):
    smem = pl.BlockSpec(memory_space=pltpu.SMEM)
    vmem = pl.BlockSpec(memory_space=pltpu.VMEM)
    width = weight.shape[1]
    return pl.pallas_call(
        lambda *refs: project_kernel(turn, *refs),
        out_shape=jax.ShapeDtypeStruct((SPAN, width), dtype),
        in_specs=[smem] + [vmem] * 5,
        out_specs=vmem,
        compiler_params=pltpu.CompilerParams(vmem_limit_bytes=16 * 1024 * 1024),
        cost_estimate=pl.CostEstimate(
            flops=2 * SPAN * 2048 * width, bytes_accessed=2048 * width * 2, transcendentals=0
        ),
        name="project",
    )(coords, *o_parts, weight)


def layer(queries, keys, values, span_table, doc_ids, out_weight):
    rows = queries.shape[0]
    spans = span_table.shape[0]
    x, z, y, core = (lax.axis_index(a) for a in ("x", "z", "y", "hd"))
    coords = jnp.stack([x, z, y, core]).astype(jnp.int32)
    kv = jnp.concatenate([keys.reshape(rows, RING, HEAD), values.reshape(rows, RING, HEAD)], axis=2)
    kv = kv.transpose(1, 0, 2)
    part = [lax.dynamic_index_in_dim(kv, (y + s) % RING, 0, keepdims=False) for s in range(RING)]
    part = [part[0]] + [shift(part[s], "y", s) for s in range(1, RING)]
    low, high = jnp.concatenate(part[:2], 0), jnp.concatenate(part[2:], 0)

    q_part = [
        lax.dynamic_slice_in_dim(queries, ((y + s) % RING) * 512, 512, 1) for s in range(RING)
    ]
    q_part = [q_part[0]] + [shift(q_part[s], "y", s) for s in range(1, RING)]

    def gathered(block, near_axis, far_axis):
        near = [block] + [shift(block, near_axis, s) for s in range(1, RING)]
        first, second = jnp.concatenate(near[:2], 0), jnp.concatenate(near[2:], 0)
        ahead_first = shift(first, far_axis, 1)
        behind_second = shift(second, far_axis, -1)
        ahead_second = shift(second, far_axis, 1)
        behind_first = shift(first, far_axis, -1)
        far_first = shift(ahead_first, far_axis, 1)
        far_second = shift(behind_second, far_axis, -1)
        return [first, second], [ahead_first, behind_second], [ahead_second, behind_first], [far_first, far_second]

    pieces = [a + b for a, b in zip(gathered(low, "z", "x"), gathered(high, "x", "z"))]

    docs = jnp.arange(DOCS, dtype=jnp.int32)
    starts = jnp.sum((doc_ids[None, :] < docs[:, None]).astype(jnp.int32), axis=1)
    slot = jnp.arange(spans, dtype=jnp.int32)
    cp = slot // 2
    dx, dz, dy = (x - cp // 16) % RING, (z - (cp // 4) % 4) % RING, (y - cp % 4) % RING
    far, near = jnp.where(dy < 2, dx, dz), jnp.where(dy < 2, dz, dx)
    early = (far == 1) == (near < 2)
    phase_of = jnp.where(far == 0, 0, jnp.where(far == 2, 3, jnp.where(early, 1, 2)))
    before = span_table[None, :] < jnp.arange(spans + 8, dtype=jnp.int32)[:, None]
    ranks = [jnp.sum((before & (phase_of == p)[None, :]).astype(jnp.int32), axis=1) for p in range(4)]

    scalars = [coords, span_table, starts]
    q_all, best, acc, weight = run_phase(0, scalars + [ranks[0]], pieces[0], q_part, out_weight)
    best, acc = run_phase(1, scalars + [ranks[1]], pieces[1], [q_all, best, acc])
    best, acc = run_phase(2, scalars + [ranks[2]], pieces[2], [q_all, best, acc])
    o_part = run_phase(3, scalars + [ranks[3]], pieces[3], [q_all, best, acc])[2:]

    def returned(part):
        return [part[0], shift(part[1], "y", -1), both, shift(part[2], "y", 1)]

    both = shift(o_part[6], "y", -2)
    theirs, ours = returned(o_part[:3]), returned(o_part[3:6])
    sent = project(0, coords, theirs, weight, jnp.bfloat16)
    sent = lax.ppermute(sent, "hd", [(0, 1), (1, 0)])
    kept = project(1, coords, ours, weight, jnp.float32)
    return (kept + sent.astype(jnp.float32)).astype(jnp.bfloat16)


def solution(mesh):
    inner = Mesh(mesh.devices.reshape(RING, RING, RING, 2), ("x", "z", "y", "hd"))
    cp = ("x", "z", "y")
    return jax.shard_map(
        layer,
        mesh=inner,
        in_specs=(P(cp, "hd"), P(cp, "hd"), P(cp, "hd"), P(), P(), P("hd", None)),
        out_specs=P(cp + ("hd",), None),
        check_vma=False,
    )
```

```python
import jax
import jax.numpy as jnp
from jax import lax
from jax.experimental import pallas as pl
from jax.experimental.pallas import tpu as pltpu
from jax.sharding import Mesh, PartitionSpec as P

HEAD = 128
SPAN = 96
RING = 4
GROUP = 4
ROWS = GROUP * SPAN
DOCS = 8
LOW = -1e30
LOG2E = 1.4426950408889634
FACTOR = HEAD ** -0.5 * LOG2E
MAX_TASKS = 160
TILE = 16
COPIES = 4

PHASES = (((0, 0), (0, 1)), ((1, 0), (3, 1)), ((1, 1), (3, 0)), ((2, 0), (2, 1)))
CHUNKS = (256, 256, 256, 256)


def shift(value, axis, by):
    return lax.ppermute(value, axis, [(i, (i + by) % RING) for i in range(RING)])


def phase_kernel(phase, *refs):
    chunk = CHUNKS[phase]
    first_phase, last_phase = phase == 0, phase == 3
    order = PHASES[phase]
    refs = list(refs)

    def take(n):
        out = refs[:n]
        del refs[:n]
        return out

    coords, table, starts, rank = take(4)
    pieces = take(2 * len(order))
    if first_phase:
        q_parts = take(4)
    else:
        (q_all,) = take(1)
        take(2)
    if first_phase:
        (weight,) = take(1)
        (q_all,) = take(1)
    best_all, acc_all = take(2)
    if last_phase:
        outs = take(7)
    if first_phase:
        (weight_held,) = take(1)
        weight_sem = refs.pop()
        height = weight.shape[0] // COPIES
        weight_copies = [
            pltpu.make_async_copy(
                weight.at[pl.ds(n * height, height)], weight_held.at[pl.ds(n * height, height)], weight_sem.at[n]
            )
            for n in range(COPIES)
        ]
        for copy in weight_copies:
            copy.start()
    kv, low_all, high_all, s0, s1, p0, p1, f0, f1, task_span, task_first, task_upper = refs
    x, z, y, core = coords[0], coords[1], coords[2], coords[3]

    def slot_of(dx, dz, dy, half):
        cp = ((x + RING - dx) % RING) * 16 + ((z + RING - dz) % RING) * 4 + (y + RING - dy) % RING
        return 2 * cp + half

    for family in range(2):
        for index, (far, upper_block) in enumerate(order):
            ref = pieces[family * len(order) + index]
            for i in range(8):
                near = 2 * upper_block + i // 4
                dy = 2 * family + (i // 2) % 2
                dx, dz = (far, near) if family == 0 else (near, far)
                row = rank[table[slot_of(dx, dz, dy, i % 2)]] * SPAN
                kv[pl.ds(pl.multiple_of(row, SPAN), SPAN), :] = ref[i * SPAN : (i + 1) * SPAN, :]

    if first_phase:
        for s, ref in enumerate(q_parts):
            for half in range(2):
                for h in range(GROUP):
                    scaled = ref[half * SPAN : (half + 1) * SPAN, h * HEAD : (h + 1) * HEAD]
                    scaled = scaled.astype(jnp.float32) * FACTOR
                    main = scaled.astype(jnp.bfloat16)
                    rest = (scaled - main.astype(jnp.float32)).astype(jnp.bfloat16)
                    q_all[2 * s + half, h * SPAN : (h + 1) * SPAN, :HEAD] = main
                    q_all[2 * s + half, h * SPAN : (h + 1) * SPAN, HEAD:] = rest
        best_all[...] = jnp.full(best_all.shape, LOW, jnp.float32)
        acc_all[...] = jnp.zeros(acc_all.shape, jnp.float32)

    doc_low = []
    for d in range(DOCS):
        span = starts[d] // SPAN
        doc_low.append(rank[span] * SPAN + (rank[span + 1] - rank[span]) * (starts[d] - span * SPAN))

    def plan(i, total):
        span = table[slot_of(0, 0, i // 2, i % 2)]
        row = lax.broadcasted_iota(jnp.int32, (SPAN, HEAD), 0)
        low = jnp.full((SPAN, HEAD), doc_low[0], jnp.int32)
        low_min = doc_low[0]
        for d in range(1, DOCS):
            low = jnp.where(row >= starts[d] - span * SPAN, doc_low[d], low)
            low_min = jnp.where(starts[d] <= span * SPAN, doc_low[d], low_min)
        low_all[i] = low
        base, top = rank[span] * SPAN, rank[span + 1] * SPAN
        high_all[i] = jnp.where(top > base, base + row, base - 1)

        def add(e, n):
            task_span[n] = i
            task_upper[n] = top - e * chunk
            task_first[n] = jnp.maximum(top - (e + 1) * chunk, 0)
            return n + 1

        return lax.fori_loop(0, (top - low_min + chunk - 1) // chunk, add, total)

    total = lax.fori_loop(0, 8, plan, 1)
    task_span[0] = 0
    task_first[0] = 0
    for extra in range(3):
        task_span[total + extra] = 0
        task_first[total + extra] = 0
        task_upper[total + extra] = 0

    p1[...] = jnp.zeros(p1.shape, jnp.bfloat16)
    f1[...] = jnp.ones(f1.shape, jnp.float32)
    ones = jnp.ones((chunk, HEAD), jnp.bfloat16)
    lanes = chunk // HEAD

    def score(t, out):
        k = kv[pl.ds(pl.multiple_of(task_first[t], 32), chunk), :HEAD]
        out[...] = lax.dot_general(
            q_all[task_span[t]], jnp.concatenate([k, k], axis=1), (((1,), (1,)), ((), ())), preferred_element_type=jnp.float32
        )

    def weigh(t, s_ref, p_ref, f_ref):
        i, k0 = task_span[t], task_first[t]
        last = task_upper[t] - 1
        lane = lax.broadcasted_iota(jnp.int32, (TILE, HEAD), 1)
        for r in range(0, SPAN, TILE):
            low = low_all[i, r : r + TILE, :] - k0
            high = jnp.minimum(high_all[i, r : r + TILE, :], last) - k0
            seen = [(lane + g * HEAD >= low) & (lane + g * HEAD <= high) for g in range(lanes)]
            for h in range(GROUP):
                at = slice(h * SPAN + r, h * SPAN + r + TILE)
                s = [
                    jnp.where(seen[g], s_ref[at, g * HEAD : (g + 1) * HEAD], 2 * LOW)
                    for g in range(lanes)
                ]
                top = s[0]
                for g in range(1, lanes):
                    top = jnp.maximum(top, s[g])
                best = best_all[i, at, :]
                new_best = jnp.maximum(best, jnp.max(top, axis=1, keepdims=True))
                best_all[i, at, :] = new_best
                f_ref[at, :] = jnp.exp2(best - new_best)
                p_ref[at, :] = jnp.concatenate([jnp.exp2(x - new_best) for x in s], axis=1).astype(
                    jnp.bfloat16
                )

    def accumulate(t, p_ref, f_ref):
        i, k0 = task_span[t], pl.multiple_of(task_first[t], 32)
        v = jnp.concatenate([kv[pl.ds(k0, chunk), HEAD:], ones], axis=1)
        part = jnp.dot(p_ref[...], v, preferred_element_type=jnp.float32)
        fade = f_ref[...]
        for half in range(2):
            cols = slice(half * HEAD, (half + 1) * HEAD)
            acc_all[i, :, cols] = acc_all[i, :, cols] * fade + part[:, cols]

    score(1, s0)

    def pair(j, _):
        t = 2 * j + 1
        accumulate(t - 1, p1, f1)
        score(t + 1, s1)
        weigh(t, s0, p0, f0)
        accumulate(t, p0, f0)
        score(t + 2, s0)
        weigh(t + 1, s1, p1, f1)
        return 0

    pairs = total // 2
    lax.fori_loop(0, pairs, pair, 0)
    accumulate(2 * pairs, p1, f1)

    if first_phase:
        for copy in weight_copies:
            copy.wait()
    if last_phase:
        for turn in range(2):
            half = 1 - core if turn == 0 else core
            for s in range(RING):
                i = 2 * s + half
                out = outs[6] if s == 2 else outs[3 * turn + min(s, 2)]
                first = turn * SPAN if s == 2 else 0
                for h in range(GROUP):
                    at = slice(h * SPAN, (h + 1) * SPAN)
                    out[first : first + SPAN, h * HEAD : (h + 1) * HEAD] = (
                        acc_all[i, at, :HEAD] / acc_all[i, at, HEAD:]
                    ).astype(jnp.bfloat16)


def run_phase(phase, scalars, pieces, others, weight=None):
    smem = pl.BlockSpec(memory_space=pltpu.SMEM)
    vmem = pl.BlockSpec(memory_space=pltpu.VMEM)
    chunk = CHUNKS[phase]
    keys = sum(piece.shape[0] for piece in pieces)
    state = [((8, ROWS, HEAD), jnp.float32), ((8, ROWS, 2 * HEAD), jnp.float32)]
    far = [] if weight is None else [weight]
    held = [(w.shape, w.dtype) for w in far]
    if phase == 0:
        outs = [((8, ROWS, 2 * HEAD), jnp.bfloat16)] + state + held
        aliases = {}
    else:
        outs = state + held
        first = 4 + len(pieces) + 1
        aliases = {first: 0, first + 1: 1}
    if phase == 3:
        part = ((SPAN, GROUP * HEAD), jnp.bfloat16)
        outs = outs + [part] * 6 + [((2 * SPAN, GROUP * HEAD), jnp.bfloat16)]
    scratch = [
        pltpu.VMEM((keys, 2 * HEAD), jnp.bfloat16),
        pltpu.VMEM((8, SPAN, HEAD), jnp.int32),
        pltpu.VMEM((8, SPAN, HEAD), jnp.int32),
        pltpu.VMEM((ROWS, chunk), jnp.float32),
        pltpu.VMEM((ROWS, chunk), jnp.float32),
        pltpu.VMEM((ROWS, chunk), jnp.bfloat16),
        pltpu.VMEM((ROWS, chunk), jnp.bfloat16),
        pltpu.VMEM((ROWS, HEAD), jnp.float32),
        pltpu.VMEM((ROWS, HEAD), jnp.float32),
        pltpu.SMEM((MAX_TASKS,), jnp.int32),
        pltpu.SMEM((MAX_TASKS,), jnp.int32),
        pltpu.SMEM((MAX_TASKS,), jnp.int32),
    ] + [pltpu.SemaphoreType.DMA((COPIES,))] * len(far)
    share = len(pieces) / 16
    return pl.pallas_call(
        lambda *refs: phase_kernel(phase, *refs),
        out_shape=[jax.ShapeDtypeStruct(*o) for o in outs],
        in_specs=[smem] * 4
        + [vmem] * (len(pieces) + len(others))
        + [pl.BlockSpec(memory_space=pltpu.HBM)] * len(far),
        out_specs=[vmem] * len(outs),
        scratch_shapes=scratch,
        input_output_aliases=aliases,
        compiler_params=pltpu.CompilerParams(vmem_limit_bytes=16 * 1024 * 1024),
        cost_estimate=pl.CostEstimate(
            flops=int(8e9 * share), bytes_accessed=int(1e7 * share), transcendentals=int(1e7 * share)
        ),
    )(*scalars, *pieces, *others, *far)


def own_kernel(coords, theirs, ours, w, out):
    block = 512
    row = pl.multiple_of(coords[2] * 512, 512)
    both = jnp.concatenate([theirs[...], ours[...]], axis=0)
    for n in range(w.shape[1] // block):
        cols = slice(n * block, (n + 1) * block)
        out[:, cols] = jnp.dot(both, w[pl.ds(row, 512), cols], preferred_element_type=jnp.float32)


def project_kernel(turn, coords, own, o1, o2, o3, w, out):
    y = coords[2]
    block = 512
    at = slice(turn * SPAN, (turn + 1) * SPAN)
    for n in range(w.shape[1] // block):
        cols = slice(n * block, (n + 1) * block)
        acc = None
        for s, ref in ((1, o1), (2, o2), (3, o3)):
            row = pl.multiple_of(((y + s) % RING) * 512, 512)
            rows = ref[at, :] if s == 2 else ref[...]
            part = jnp.dot(rows, w[pl.ds(row, 512), cols], preferred_element_type=jnp.float32)
            acc = part if acc is None else acc + part
        out[:, cols] = (acc + own[at, cols]).astype(out.dtype)


def dense(kernel, coords, operands, weight, height, dtype):
    smem = pl.BlockSpec(memory_space=pltpu.SMEM)
    vmem = pl.BlockSpec(memory_space=pltpu.VMEM)
    width = weight.shape[1]
    return pl.pallas_call(
        kernel,
        out_shape=jax.ShapeDtypeStruct((height, width), dtype),
        in_specs=[smem] + [vmem] * (len(operands) + 1),
        out_specs=vmem,
        compiler_params=pltpu.CompilerParams(vmem_limit_bytes=16 * 1024 * 1024),
        cost_estimate=pl.CostEstimate(
            flops=2 * SPAN * 2048 * width, bytes_accessed=2048 * width * 2, transcendentals=0
        ),
    )(coords, *operands, weight)


def project(turn, coords, operands, weight, dtype):
    return dense(lambda *refs: project_kernel(turn, *refs), coords, operands, weight, SPAN, dtype)


def layer(queries, keys, values, span_table, doc_ids, out_weight):
    rows = queries.shape[0]
    spans = span_table.shape[0]
    x, z, y, core = (lax.axis_index(a) for a in ("x", "z", "y", "hd"))
    coords = jnp.stack([x, z, y, core]).astype(jnp.int32)
    kv = jnp.concatenate([keys.reshape(rows, RING, HEAD), values.reshape(rows, RING, HEAD)], axis=2)
    kv = kv.transpose(1, 0, 2)
    part = [lax.dynamic_index_in_dim(kv, (y + s) % RING, 0, keepdims=False) for s in range(RING)]
    part = [part[0]] + [shift(part[s], "y", s) for s in range(1, RING)]
    low, high = jnp.concatenate(part[:2], 0), jnp.concatenate(part[2:], 0)

    q_part = [
        lax.dynamic_slice_in_dim(queries, ((y + s) % RING) * 512, 512, 1) for s in range(RING)
    ]
    q_part = [q_part[0]] + [shift(q_part[s], "y", s) for s in range(1, RING)]

    def gathered(block, near_axis, far_axis):
        near = [block] + [shift(block, near_axis, s) for s in range(1, RING)]
        first, second = jnp.concatenate(near[:2], 0), jnp.concatenate(near[2:], 0)
        ahead_first = shift(first, far_axis, 1)
        behind_second = shift(second, far_axis, -1)
        ahead_second = shift(second, far_axis, 1)
        behind_first = shift(first, far_axis, -1)
        far_first = shift(ahead_first, far_axis, 1)
        far_second = shift(behind_second, far_axis, -1)
        return [first, second], [ahead_first, behind_second], [ahead_second, behind_first], [far_first, far_second]

    pieces = [a + b for a, b in zip(gathered(low, "z", "x"), gathered(high, "x", "z"))]

    docs = jnp.arange(DOCS, dtype=jnp.int32)
    starts = jnp.sum((doc_ids[None, :] < docs[:, None]).astype(jnp.int32), axis=1)
    slot = jnp.arange(spans, dtype=jnp.int32)
    cp = slot // 2
    dx, dz, dy = (x - cp // 16) % RING, (z - (cp // 4) % 4) % RING, (y - cp % 4) % RING
    far, near = jnp.where(dy < 2, dx, dz), jnp.where(dy < 2, dz, dx)
    early = (far == 1) == (near < 2)
    phase_of = jnp.where(far == 0, 0, jnp.where(far == 2, 3, jnp.where(early, 1, 2)))
    before = span_table[None, :] < jnp.arange(spans + 8, dtype=jnp.int32)[:, None]
    ranks = [jnp.sum((before & (phase_of == p)[None, :]).astype(jnp.int32), axis=1) for p in range(4)]

    scalars = [coords, span_table, starts]
    q_all, best, acc, weight = run_phase(0, scalars + [ranks[0]], pieces[0], q_part, out_weight)
    best, acc = run_phase(1, scalars + [ranks[1]], pieces[1], [q_all, best, acc])
    best, acc = run_phase(2, scalars + [ranks[2]], pieces[2], [q_all, best, acc])
    o_part = run_phase(3, scalars + [ranks[3]], pieces[3], [q_all, best, acc])[2:]

    def returned(part):
        return [own, shift(part[1], "y", -1), both, shift(part[2], "y", 1)]

    both = shift(o_part[6], "y", -2)
    own = dense(own_kernel, coords, [o_part[0], o_part[3]], weight, 2 * SPAN, jnp.float32)
    theirs, ours = returned(o_part[:3]), returned(o_part[3:6])
    sent = project(0, coords, theirs, weight, jnp.bfloat16)
    sent = lax.ppermute(sent, "hd", [(0, 1), (1, 0)])
    kept = project(1, coords, ours, weight, jnp.float32)
    return (kept + sent.astype(jnp.float32)).astype(jnp.bfloat16)


def solution(mesh):
    inner = Mesh(mesh.devices.reshape(RING, RING, RING, 2), ("x", "z", "y", "hd"))
    cp = ("x", "z", "y")
    return jax.shard_map(
        layer,
        mesh=inner,
        in_specs=(P(cp, "hd"), P(cp, "hd"), P(cp, "hd"), P(), P(), P("hd", None)),
        out_specs=P(cp + ("hd",), None),
        check_vma=False,
    )
```

```python
import jax
import jax.numpy as jnp
from jax import lax
from jax.experimental import pallas as pl
from jax.experimental.pallas import tpu as pltpu
from jax.sharding import Mesh, PartitionSpec as P

HEAD = 128
SPAN = 96
RING = 4
GROUP = 4
ROWS = GROUP * SPAN
DOCS = 8
LOW = -1e30
LOG2E = 1.4426950408889634
FACTOR = HEAD ** -0.5 * LOG2E
MAX_TASKS = 160
TILE = 16
COPIES = 4
UNROLL = 4

PHASES = (((0, 0), (0, 1)), ((1, 0), (3, 1)), ((1, 1), (3, 0)), ((2, 0), (2, 1)))
CHUNKS = (256, 256, 256, 256)


def shift(value, axis, by):
    return lax.ppermute(value, axis, [(i, (i + by) % RING) for i in range(RING)])


def phase_kernel(phase, *refs):
    chunk = CHUNKS[phase]
    first_phase, last_phase = phase == 0, phase == 3
    order = PHASES[phase]
    refs = list(refs)

    def take(n):
        out = refs[:n]
        del refs[:n]
        return out

    coords, table, starts, rank = take(4)
    pieces = take(2 * len(order))
    if first_phase:
        q_parts = take(4)
    else:
        (q_all,) = take(1)
        take(2)
    if first_phase:
        (weight,) = take(1)
        (q_all,) = take(1)
    best_all, acc_all = take(2)
    if last_phase:
        outs = take(7)
    if first_phase:
        (weight_held,) = take(1)
        weight_sem = refs.pop()
        height = weight.shape[0] // COPIES
        weight_copies = [
            pltpu.make_async_copy(
                weight.at[pl.ds(n * height, height)], weight_held.at[pl.ds(n * height, height)], weight_sem.at[n]
            )
            for n in range(COPIES)
        ]
        for copy in weight_copies:
            copy.start()
    kv, low_all, high_all, s0, s1, p0, p1, f0, f1, task_span, task_first, task_upper = refs
    x, z, y, core = coords[0], coords[1], coords[2], coords[3]

    def slot_of(dx, dz, dy, half):
        cp = ((x + RING - dx) % RING) * 16 + ((z + RING - dz) % RING) * 4 + (y + RING - dy) % RING
        return 2 * cp + half

    for family in range(2):
        for index, (far, upper_block) in enumerate(order):
            ref = pieces[family * len(order) + index]
            for i in range(8):
                near = 2 * upper_block + i // 4
                dy = 2 * family + (i // 2) % 2
                dx, dz = (far, near) if family == 0 else (near, far)
                row = rank[table[slot_of(dx, dz, dy, i % 2)]] * SPAN
                kv[pl.ds(pl.multiple_of(row, SPAN), SPAN), :] = ref[i * SPAN : (i + 1) * SPAN, :]

    if first_phase:
        for s, ref in enumerate(q_parts):
            for half in range(2):
                for h in range(GROUP):
                    scaled = ref[half * SPAN : (half + 1) * SPAN, h * HEAD : (h + 1) * HEAD]
                    scaled = scaled.astype(jnp.float32) * FACTOR
                    main = scaled.astype(jnp.bfloat16)
                    rest = (scaled - main.astype(jnp.float32)).astype(jnp.bfloat16)
                    q_all[2 * s + half, h * SPAN : (h + 1) * SPAN, :HEAD] = main
                    q_all[2 * s + half, h * SPAN : (h + 1) * SPAN, HEAD:] = rest
        best_all[...] = jnp.full(best_all.shape, LOW, jnp.float32)
        acc_all[...] = jnp.zeros(acc_all.shape, jnp.float32)

    doc_low = []
    for d in range(DOCS):
        span = starts[d] // SPAN
        doc_low.append(rank[span] * SPAN + (rank[span + 1] - rank[span]) * (starts[d] - span * SPAN))

    def plan(i, total):
        span = table[slot_of(0, 0, i // 2, i % 2)]
        row = lax.broadcasted_iota(jnp.int32, (SPAN, HEAD), 0)
        low = jnp.full((SPAN, HEAD), doc_low[0], jnp.int32)
        low_min = doc_low[0]
        for d in range(1, DOCS):
            low = jnp.where(row >= starts[d] - span * SPAN, doc_low[d], low)
            low_min = jnp.where(starts[d] <= span * SPAN, doc_low[d], low_min)
        low_all[i] = low
        base, top = rank[span] * SPAN, rank[span + 1] * SPAN
        high_all[i] = jnp.where(top > base, base + row, base - 1)

        def add(e, n):
            task_span[n] = i
            task_upper[n] = top - e * chunk
            task_first[n] = jnp.maximum(top - (e + 1) * chunk, 0)
            return n + 1

        return lax.fori_loop(0, (top - low_min + chunk - 1) // chunk, add, total)

    total = lax.fori_loop(0, 8, plan, 1)
    task_span[0] = 0
    task_first[0] = 0
    for extra in range(UNROLL + 1):
        task_span[total + extra] = 0
        task_first[total + extra] = 0
        task_upper[total + extra] = 0

    p1[...] = jnp.zeros(p1.shape, jnp.bfloat16)
    f1[...] = jnp.ones(f1.shape, jnp.float32)
    ones = jnp.ones((chunk, HEAD), jnp.bfloat16)
    lanes = chunk // HEAD

    def score(t, out):
        k = kv[pl.ds(pl.multiple_of(task_first[t], 32), chunk), :HEAD]
        out[...] = lax.dot_general(
            q_all[task_span[t]], jnp.concatenate([k, k], axis=1), (((1,), (1,)), ((), ())), preferred_element_type=jnp.float32
        )

    def weigh(t, s_ref, p_ref, f_ref):
        i, k0 = task_span[t], task_first[t]
        last = task_upper[t] - 1
        lane = lax.broadcasted_iota(jnp.int32, (TILE, HEAD), 1)
        for r in range(0, SPAN, TILE):
            low = low_all[i, r : r + TILE, :] - k0
            high = jnp.minimum(high_all[i, r : r + TILE, :], last) - k0
            seen = [(lane + g * HEAD >= low) & (lane + g * HEAD <= high) for g in range(lanes)]
            for h in range(GROUP):
                at = slice(h * SPAN + r, h * SPAN + r + TILE)
                s = [
                    jnp.where(seen[g], s_ref[at, g * HEAD : (g + 1) * HEAD], 2 * LOW)
                    for g in range(lanes)
                ]
                top = s[0]
                for g in range(1, lanes):
                    top = jnp.maximum(top, s[g])
                best = best_all[i, at, :]
                new_best = jnp.maximum(best, jnp.max(top, axis=1, keepdims=True))
                best_all[i, at, :] = new_best
                f_ref[at, :] = jnp.exp2(best - new_best)
                p_ref[at, :] = jnp.concatenate([jnp.exp2(x - new_best) for x in s], axis=1).astype(
                    jnp.bfloat16
                )

    def accumulate(t, p_ref, f_ref):
        i, k0 = task_span[t], pl.multiple_of(task_first[t], 32)
        v = jnp.concatenate([kv[pl.ds(k0, chunk), HEAD:], ones], axis=1)
        part = jnp.dot(p_ref[...], v, preferred_element_type=jnp.float32)
        fade = f_ref[...]
        for half in range(2):
            cols = slice(half * HEAD, (half + 1) * HEAD)
            acc_all[i, :, cols] = acc_all[i, :, cols] * fade + part[:, cols]

    score(1, s0)

    def several(j, _):
        for u in range(0, UNROLL, 2):
            t = UNROLL * j + 1 + u
            accumulate(t - 1, p1, f1)
            score(t + 1, s1)
            weigh(t, s0, p0, f0)
            accumulate(t, p0, f0)
            score(t + 2, s0)
            weigh(t + 1, s1, p1, f1)
        return 0

    rounds = (total - 1 + UNROLL - 1) // UNROLL
    lax.fori_loop(0, rounds, several, 0)
    accumulate(UNROLL * rounds, p1, f1)

    if first_phase:
        for copy in weight_copies:
            copy.wait()
    if last_phase:
        for turn in range(2):
            half = 1 - core if turn == 0 else core
            for s in range(RING):
                i = 2 * s + half
                out = outs[6] if s == 2 else outs[3 * turn + min(s, 2)]
                first = turn * SPAN if s == 2 else 0
                for h in range(GROUP):
                    at = slice(h * SPAN, (h + 1) * SPAN)
                    out[first : first + SPAN, h * HEAD : (h + 1) * HEAD] = (
                        acc_all[i, at, :HEAD] / acc_all[i, at, HEAD:]
                    ).astype(jnp.bfloat16)


def run_phase(phase, scalars, pieces, others, weight=None):
    smem = pl.BlockSpec(memory_space=pltpu.SMEM)
    vmem = pl.BlockSpec(memory_space=pltpu.VMEM)
    chunk = CHUNKS[phase]
    keys = sum(piece.shape[0] for piece in pieces)
    state = [((8, ROWS, HEAD), jnp.float32), ((8, ROWS, 2 * HEAD), jnp.float32)]
    far = [] if weight is None else [weight]
    held = [(w.shape, w.dtype) for w in far]
    if phase == 0:
        outs = [((8, ROWS, 2 * HEAD), jnp.bfloat16)] + state + held
        aliases = {}
    else:
        outs = state + held
        first = 4 + len(pieces) + 1
        aliases = {first: 0, first + 1: 1}
    if phase == 3:
        part = ((SPAN, GROUP * HEAD), jnp.bfloat16)
        outs = outs + [part] * 6 + [((2 * SPAN, GROUP * HEAD), jnp.bfloat16)]
    scratch = [
        pltpu.VMEM((keys, 2 * HEAD), jnp.bfloat16),
        pltpu.VMEM((8, SPAN, HEAD), jnp.int32),
        pltpu.VMEM((8, SPAN, HEAD), jnp.int32),
        pltpu.VMEM((ROWS, chunk), jnp.float32),
        pltpu.VMEM((ROWS, chunk), jnp.float32),
        pltpu.VMEM((ROWS, chunk), jnp.bfloat16),
        pltpu.VMEM((ROWS, chunk), jnp.bfloat16),
        pltpu.VMEM((ROWS, HEAD), jnp.float32),
        pltpu.VMEM((ROWS, HEAD), jnp.float32),
        pltpu.SMEM((MAX_TASKS,), jnp.int32),
        pltpu.SMEM((MAX_TASKS,), jnp.int32),
        pltpu.SMEM((MAX_TASKS,), jnp.int32),
    ] + [pltpu.SemaphoreType.DMA((COPIES,))] * len(far)
    share = len(pieces) / 16
    return pl.pallas_call(
        lambda *refs: phase_kernel(phase, *refs),
        out_shape=[jax.ShapeDtypeStruct(*o) for o in outs],
        in_specs=[smem] * 4
        + [vmem] * (len(pieces) + len(others))
        + [pl.BlockSpec(memory_space=pltpu.HBM)] * len(far),
        out_specs=[vmem] * len(outs),
        scratch_shapes=scratch,
        input_output_aliases=aliases,
        compiler_params=pltpu.CompilerParams(vmem_limit_bytes=16 * 1024 * 1024),
        cost_estimate=pl.CostEstimate(
            flops=int(8e9 * share), bytes_accessed=int(1e7 * share), transcendentals=int(1e7 * share)
        ),
    )(*scalars, *pieces, *others, *far)


def own_kernel(coords, theirs, ours, w, out):
    block = 512
    row = pl.multiple_of(coords[2] * 512, 512)
    both = jnp.concatenate([theirs[...], ours[...]], axis=0)
    for n in range(w.shape[1] // block):
        cols = slice(n * block, (n + 1) * block)
        out[:, cols] = jnp.dot(both, w[pl.ds(row, 512), cols], preferred_element_type=jnp.float32)


def project_kernel(turn, coords, own, o1, o2, o3, w, out):
    y = coords[2]
    block = 512
    at = slice(turn * SPAN, (turn + 1) * SPAN)
    for n in range(w.shape[1] // block):
        cols = slice(n * block, (n + 1) * block)
        acc = None
        for s, ref in ((1, o1), (2, o2), (3, o3)):
            row = pl.multiple_of(((y + s) % RING) * 512, 512)
            rows = ref[at, :] if s == 2 else ref[...]
            part = jnp.dot(rows, w[pl.ds(row, 512), cols], preferred_element_type=jnp.float32)
            acc = part if acc is None else acc + part
        out[:, cols] = (acc + own[at, cols]).astype(out.dtype)


def dense(kernel, coords, operands, weight, height, dtype):
    smem = pl.BlockSpec(memory_space=pltpu.SMEM)
    vmem = pl.BlockSpec(memory_space=pltpu.VMEM)
    width = weight.shape[1]
    return pl.pallas_call(
        kernel,
        out_shape=jax.ShapeDtypeStruct((height, width), dtype),
        in_specs=[smem] + [vmem] * (len(operands) + 1),
        out_specs=vmem,
        compiler_params=pltpu.CompilerParams(vmem_limit_bytes=16 * 1024 * 1024),
        cost_estimate=pl.CostEstimate(
            flops=2 * SPAN * 2048 * width, bytes_accessed=2048 * width * 2, transcendentals=0
        ),
    )(coords, *operands, weight)


def project(turn, coords, operands, weight, dtype):
    return dense(lambda *refs: project_kernel(turn, *refs), coords, operands, weight, SPAN, dtype)


def layer(queries, keys, values, span_table, doc_ids, out_weight):
    spans = span_table.shape[0]
    x, z, y, core = (lax.axis_index(a) for a in ("x", "z", "y", "hd"))
    coords = jnp.stack([x, z, y, core]).astype(jnp.int32)
    rows = queries.shape[0]
    kv = jnp.concatenate([keys.reshape(rows, RING, HEAD), values.reshape(rows, RING, HEAD)], axis=2)
    kv = kv.transpose(1, 0, 2)
    part = [lax.dynamic_index_in_dim(kv, (y + s) % RING, 0, keepdims=False) for s in range(RING)]
    part = [part[0]] + [shift(part[s], "y", s) for s in range(1, RING)]
    low, high = jnp.concatenate(part[:2], 0), jnp.concatenate(part[2:], 0)

    q_part = [
        lax.dynamic_slice_in_dim(queries, ((y + s) % RING) * 512, 512, 1) for s in range(RING)
    ]
    q_part = [q_part[0]] + [shift(q_part[s], "y", s) for s in range(1, RING)]

    def gathered(block, near_axis, far_axis):
        near = [block] + [shift(block, near_axis, s) for s in range(1, RING)]
        first, second = jnp.concatenate(near[:2], 0), jnp.concatenate(near[2:], 0)
        ahead_first = shift(first, far_axis, 1)
        behind_second = shift(second, far_axis, -1)
        ahead_second = shift(second, far_axis, 1)
        behind_first = shift(first, far_axis, -1)
        far_first = shift(ahead_first, far_axis, 1)
        far_second = shift(behind_second, far_axis, -1)
        return [first, second], [ahead_first, behind_second], [ahead_second, behind_first], [far_first, far_second]

    pieces = [a + b for a, b in zip(gathered(low, "z", "x"), gathered(high, "x", "z"))]

    docs = jnp.arange(DOCS, dtype=jnp.int32)
    starts = jnp.sum((doc_ids[None, :] < docs[:, None]).astype(jnp.int32), axis=1)
    slot = jnp.arange(spans, dtype=jnp.int32)
    cp = slot // 2
    dx, dz, dy = (x - cp // 16) % RING, (z - (cp // 4) % 4) % RING, (y - cp % 4) % RING
    far, near = jnp.where(dy < 2, dx, dz), jnp.where(dy < 2, dz, dx)
    early = (far == 1) == (near < 2)
    phase_of = jnp.where(far == 0, 0, jnp.where(far == 2, 3, jnp.where(early, 1, 2)))
    before = span_table[None, :] < jnp.arange(spans + 8, dtype=jnp.int32)[:, None]
    ranks = [jnp.sum((before & (phase_of == p)[None, :]).astype(jnp.int32), axis=1) for p in range(4)]

    scalars = [coords, span_table, starts]
    q_all, best, acc, weight = run_phase(0, scalars + [ranks[0]], pieces[0], q_part, out_weight)
    best, acc = run_phase(1, scalars + [ranks[1]], pieces[1], [q_all, best, acc])
    best, acc = run_phase(2, scalars + [ranks[2]], pieces[2], [q_all, best, acc])
    o_part = run_phase(3, scalars + [ranks[3]], pieces[3], [q_all, best, acc])[2:]

    def returned(part):
        return [own, shift(part[1], "y", -1), both, shift(part[2], "y", 1)]

    both = shift(o_part[6], "y", -2)
    own = dense(own_kernel, coords, [o_part[0], o_part[3]], weight, 2 * SPAN, jnp.float32)
    theirs, ours = returned(o_part[:3]), returned(o_part[3:6])
    sent = project(0, coords, theirs, weight, jnp.bfloat16)
    sent = lax.ppermute(sent, "hd", [(0, 1), (1, 0)])
    kept = project(1, coords, ours, weight, jnp.float32)
    return (kept + sent.astype(jnp.float32)).astype(jnp.bfloat16)


def solution(mesh):
    inner = Mesh(mesh.devices.reshape(RING, RING, RING, 2), ("x", "z", "y", "hd"))
    cp = ("x", "z", "y")
    return jax.shard_map(
        layer,
        mesh=inner,
        in_specs=(P(cp, "hd"), P(cp, "hd"), P(cp, "hd"), P(), P(), P("hd", None)),
        out_specs=P(cp + ("hd",), None),
        check_vma=False,
    )
```
